512 devices in a mesh: dom: 32 (over z, x), snap: 16 (over y, core).
Axes of the slice: x: 4, y: 8, z: 8, core: 2. Of those that a mesh axis runs over, the one named last changes fastest.
Arguments:
- feat: bfloat16 [16, 4096, 512], P('snap', 'dom'), may hold values from -6 to 6
- w_struct: bfloat16 [512, 1536], replicated, may hold values from -0.25 to 0.25
- w_temp: bfloat16 [512, 1536], replicated, may hold values from -0.25 to 0.25
- pos_embed: bfloat16 [16, 512], replicated, may hold values from -3 to 3
- rel_bias: float32 [4, 8], replicated, may hold values from -1.5 to 1.5
- nbr: int32 [16, 4096, 8], P('snap', 'dom'), may hold values from 0 to 383
- rel_type: int32 [16, 4096, 8], P('snap', 'dom'), may hold values from 0 to 3
- send_idx: int32 [16, 32, 32, 8], P('snap', 'dom'), may hold values from 0 to 127
- active: int32 [16, 4096], P(None, ('dom', 'snap')), may hold values 0 or 1
- cotangent: bfloat16 [16, 4096, 512], P(None, ('dom', 'snap')), may hold values from -6 to 6
Outputs:
- grad_feat: bfloat16 [16, 4096, 512], P('snap', 'dom')
- grad_wtemp: float32 [512, 1536], P('snap')
The draws below stay inside these ranges and needn't reach their ends.
Inputs may be any that keep to these rules, and one draw needn't show every extreme that they name: `nbr`: rows of the partition's key table: its 128 own entities first, then 8 halo rows from each partition in order.
All inputs are finite; a program needn't handle non-finite values. No bound on the sum of `active` on one device may be relied on, other than what follows from the above.
Results may differ from the reference program's by a relative error of at most 0.024.
Values may be sent and summed in bfloat16 or wider, within the bound.
A program may use at most 64 MiB of HBM per device.

```python
import jax
import jax.numpy as jnp
from jax import lax

D = 512
HEADS = 8
REL = 4
DEG = 8
PEER = 8
ENT_DEV = 128
ENTITIES = 4096
SNAPS = 16
KEYS = 384
N_DOM = 32


def place_ends(entries, rng, low, high):
    shape = entries.shape
    place = [jax.random.randint(jax.random.fold_in(rng, axis), (), 0, shape[axis]) for axis in range(len(shape))]
    entries = entries.at[tuple(place)].set(low)
    longest = shape.index(max(shape))
    place[longest] = (place[longest] + 1) % shape[longest]
    return entries.at[tuple(place)].set(high)


def block_scale(stream_key, shape, shards, least, high):
    def one(position, blocks):
        steps = jax.random.uniform(jax.random.fold_in(jax.random.fold_in(stream_key, 6), position), (blocks,), jnp.float32, least / len(shards), high / len(shards))
        return jnp.repeat(jnp.exp(steps), shape[position] // blocks).reshape((-1,) + (1,) * (len(shape) - position - 1))

    loudness = one(*shards[0])
    for cut in shards[1:]:
        loudness = loudness * one(*cut)
    return loudness


def noise(stream_key, dims, deviation, reach, shards=(), held_as=jnp.bfloat16):
    gain = block_scale(stream_key, dims, shards, -0.22, 0.18) if shards else 1.0
    result = jax.random.normal(stream_key, dims, jnp.float32) * deviation * gain
    return jnp.minimum(jnp.maximum(result, -reach), reach).astype(held_as)


def setup_inputs(seed: int = 0) -> dict:
    streams_of = jax.random.split(jax.random.key(seed), 11)
    feat = noise(streams_of[0], (SNAPS, ENTITIES, D), 1.0, 6.0, ((0, 16), (1, 32)))
    w_struct = noise(streams_of[1], (D, 3 * D), D ** -0.5, 0.25)
    w_temp = noise(streams_of[2], (D, 3 * D), D ** -0.5, 0.25)
    pos_embed = noise(streams_of[3], (SNAPS, D), 0.5, 3.0)
    rel_bias = jnp.clip(jax.random.uniform(streams_of[4], (REL, HEADS), jnp.float32, -1.5, 1.5), -1.5, 1.5)
    nbr = place_ends(jax.random.randint(streams_of[5], (SNAPS, ENTITIES, DEG), 0, KEYS), jax.random.fold_in(streams_of[5], 1), 0, KEYS - 1).astype(jnp.int32)
    rel_type = place_ends(jax.random.randint(streams_of[6], (SNAPS, ENTITIES, DEG), 0, REL), jax.random.fold_in(streams_of[6], 1), 0, REL - 1).astype(jnp.int32)
    send_idx = place_ends(jax.random.randint(streams_of[7], (SNAPS, N_DOM, N_DOM, PEER), 0, ENT_DEV), jax.random.fold_in(streams_of[7], 1), 0, ENT_DEV - 1).astype(jnp.int32)
    active = place_ends((jax.random.randint(streams_of[8], (SNAPS, ENTITIES), 0, 4) < 3).astype(jnp.int32), jax.random.fold_in(streams_of[8], 1), 0, 1)
    cotangent = noise(streams_of[9], (SNAPS, ENTITIES, D), 1.0, 6.0, ((1, 512),))
    return {"feat": feat, "w_struct": w_struct, "w_temp": w_temp, "pos_embed": pos_embed, "rel_bias": rel_bias, "nbr": nbr, "rel_type": rel_type, "send_idx": send_idx, "active": active, "cotangent": cotangent}


def edge_scores(rel_ids, rel_bias):
    onehot = (rel_ids[..., None] == jnp.arange(rel_bias.shape[0], dtype=jnp.int32)).astype(jnp.float32)
    return jnp.einsum('rek,kh->reh', onehot, rel_bias.astype(jnp.float32), precision=lax.Precision.HIGHEST)

def struct_core(query, key_tab, val_tab, links, edge_add):
    row_count, width = query.shape
    slots = links.shape[1]
    head_dim = width // HEADS
    keys_g = key_tab[links].reshape(row_count, slots, HEADS, head_dim)
    vals_g = val_tab[links].reshape(row_count, slots, HEADS, head_dim)
    query_h = query.reshape(row_count, HEADS, head_dim)
    scores = jnp.einsum('rhc,rehc->reh', query_h, keys_g) * head_dim ** (-0.5) + edge_add
    weights = jax.nn.softmax(scores, axis=1)
    rounded = lax.optimization_barrier(weights.astype(jnp.bfloat16)).astype(jnp.float32)
    return jnp.einsum('reh,rehc->rhc', rounded, vals_g).reshape(row_count, width)

def temp_allowed(active_blk):
    snaps = active_blk.shape[0]
    later = jnp.arange(snaps, dtype=jnp.int32)[:, None]
    earlier = jnp.arange(snaps, dtype=jnp.int32)[None, :]
    causal = (earlier <= later)[..., None]
    itself = (earlier == later)[..., None]
    return causal & (itself | (active_blk[None, :, :] == 1))

def temp_core(t_query, t_key, t_value, allowed):
    snaps, count, width = t_query.shape
    head_dim = width // HEADS
    query_h = t_query.reshape(snaps, count, HEADS, head_dim)
    key_h = t_key.reshape(snaps, count, HEADS, head_dim)
    value_h = t_value.reshape(snaps, count, HEADS, head_dim)
    scores = jnp.einsum('tmhc,umhc->tumh', query_h, key_h) * head_dim ** (-0.5)
    scores = jnp.where(allowed[..., None], scores, -1e+30)
    weights = jax.nn.softmax(scores, axis=1)
    rounded = lax.optimization_barrier(weights.astype(jnp.bfloat16)).astype(jnp.float32)
    return jnp.einsum('tumh,umhc->tmhc', rounded, value_h).reshape(snaps, count, width)

def reference(feat, w_struct, w_temp, pos_embed, rel_bias, nbr, rel_type, send_idx, active, cotangent):
    width = D
    cot_f = cotangent.astype(jnp.float32)

    def halo_index(send_s):
        offsets = (jnp.arange(N_DOM, dtype=jnp.int32) * ENT_DEV)[:, None, None]
        return jnp.transpose(send_s + offsets, (1, 0, 2)).reshape(N_DOM, N_DOM * PEER)

    def struct_inputs(x_snap, send_s):
        proj = jnp.dot(x_snap, w_struct, preferred_element_type=jnp.float32).astype(jnp.bfloat16)
        query = proj[:, :width].astype(jnp.float32).reshape(N_DOM, ENT_DEV, width)
        pairs = proj[:, width:]
        halo_ids = halo_index(send_s)
        owned = pairs.reshape(N_DOM, ENT_DEV, 2 * width)
        table = jnp.concatenate([owned, pairs[halo_ids]], axis=1).astype(jnp.float32)
        return (query, table, halo_ids)

    def forward_snap(items):
        x_snap, nbr_s, rel_s, send_s = items
        query, table, halo_ids = struct_inputs(x_snap, send_s)
        edge_add = edge_scores(rel_s, rel_bias).reshape(N_DOM, ENT_DEV, DEG, HEADS)
        links = nbr_s.reshape(N_DOM, ENT_DEV, DEG)
        summed = lax.map(lambda part: struct_core(part[0], part[1][:, :width], part[1][:, width:], part[2], part[3]), (query, table, links, edge_add)).reshape(ENTITIES, width)
        hidden = (x_snap.astype(jnp.float32) + jax.nn.elu(summed)).astype(jnp.bfloat16)
        return (hidden, summed)
    hstruct, aggs = lax.map(forward_snap, (feat, nbr, rel_type, send_idx))
    z_in = (hstruct.astype(jnp.float32) + pos_embed.astype(jnp.float32)[:, None, :]).astype(jnp.bfloat16)
    z_flat = z_in.reshape(-1, width)
    t_proj = jnp.dot(z_flat, w_temp, preferred_element_type=jnp.float32).astype(jnp.bfloat16)
    t_proj = t_proj.reshape(SNAPS, ENTITIES, 3 * width).astype(jnp.float32)
    allowed = temp_allowed(active)
    _, pull = jax.vjp(lambda a_in, b_in, c_in: temp_core(a_in, b_in, c_in, allowed), t_proj[..., :width], t_proj[..., width:2 * width], t_proj[..., 2 * width:])
    grads_t = pull(cot_f)
    dt_proj = jnp.concatenate(grads_t, axis=-1).astype(jnp.bfloat16).reshape(-1, 3 * width)
    grad_wtemp = lax.dot_general(z_flat, dt_proj, (((0,), (0,)), ((), ())), preferred_element_type=jnp.float32)
    d_z = cot_f + jnp.dot(dt_proj, w_temp.T, preferred_element_type=jnp.float32).reshape(SNAPS, ENTITIES, width)
    d_hidden = d_z.astype(jnp.bfloat16)

    def backward_snap(items):
        x_snap, nbr_s, rel_s, send_s, agg_s, dh_s = items
        query, table, halo_ids = struct_inputs(x_snap, send_s)
        edge_add = edge_scores(rel_s, rel_bias).reshape(N_DOM, ENT_DEV, DEG, HEADS)
        links = nbr_s.reshape(N_DOM, ENT_DEV, DEG)
        dh_f = dh_s.astype(jnp.float32)
        d_agg = (dh_f * jnp.where(agg_s > 0, 1.0, jnp.exp(agg_s))).reshape(N_DOM, ENT_DEV, width)

        def one_part(part):
            query_p, table_p, links_p, edge_p, grad_p = part
            _, pull_p = jax.vjp(lambda a_in, b_in, c_in: struct_core(a_in, b_in, c_in, links_p, edge_p), query_p, table_p[:, :width], table_p[:, width:])
            return pull_p(grad_p)
        d_query, d_key, d_val = lax.map(one_part, (query, table, links, edge_add, d_agg))
        d_pairs = jnp.concatenate([d_key, d_val], axis=-1)
        summed = d_pairs[:, :ENT_DEV].reshape(ENTITIES, 2 * width)
        summed = summed.at[halo_ids.reshape(-1)].add(d_pairs[:, ENT_DEV:].reshape(-1, 2 * width))
        d_proj = jnp.concatenate([d_query.reshape(ENTITIES, width), summed], axis=-1).astype(jnp.bfloat16)
        return (dh_f + jnp.dot(d_proj, w_struct.T, preferred_element_type=jnp.float32)).astype(jnp.bfloat16)
    grad_feat = lax.map(backward_snap, (feat, nbr, rel_type, send_idx, aggs, d_hidden))
    return (grad_feat, grad_wtemp)
```

```python
import functools

import jax
import jax.numpy as jnp
from jax import lax
from jax.experimental import pallas as pl
from jax.experimental.pallas import tpu as pltpu
from jax.sharding import PartitionSpec as P

HEADS = 8
MESH = pl.DeviceIdType.MESH
BF = jnp.bfloat16
F32 = jnp.float32
GRID = {32: (8, 4), 4: (2, 2)}


def mm(a, b):
    return jnp.dot(a, b, preferred_element_type=F32)


def mm_nt(a, b):
    return lax.dot_general(a, b, (((1,), (1,)), ((), ())), preferred_element_type=F32)


def mm_tn(a, b):
    return lax.dot_general(a, b, (((0,), (0,)), ((), ())), preferred_element_type=F32)


def iota(shape, axis):
    return lax.broadcasted_iota(jnp.int32, shape, axis)


def where_bf(mask, value):
    return jnp.where(mask, value, jnp.zeros_like(value))


def copy_to(src, dst, send_sem, recv_sem, device):
    return pltpu.make_async_remote_copy(
        src_ref=src,
        dst_ref=dst,
        send_sem=send_sem,
        recv_sem=recv_sem,
        device_id=device,
        device_id_type=MESH,
    )


class Exchange:
    def __init__(self, count, me, device_of, src, dst, sems):
        self.count, self.me, self.device_of = count, me, device_of
        self.src, self.dst, self.send, self.recv = src, dst, sems.at[0], sems.at[1]

    def each(self, act):
        def body(step, carry):
            peer = lax.rem(self.me + step, self.count)
            act(peer)
            return carry

        lax.fori_loop(1, self.count, body, 0)

    def start(self):
        self.each(
            lambda peer: copy_to(
                self.src(peer),
                self.dst.at[self.me],
                self.send.at[peer],
                self.recv.at[self.me],
                self.device_of(peer),
            ).start()
        )

    def wait_recv(self):
        self.each(
            lambda peer: copy_to(
                self.src(peer),
                self.dst.at[peer],
                self.send.at[peer],
                self.recv.at[peer],
                self.device_of(peer),
            ).wait_recv()
        )

    def wait_send(self):
        self.each(
            lambda peer: copy_to(
                self.src(peer),
                self.dst.at[peer],
                self.send.at[peer],
                self.recv.at[peer],
                self.device_of(peer),
            ).wait_send()
        )


def kernel(
    sizes,
    x_ref,
    ws_ref,
    wt_ref,
    pos_ref,
    rb_ref,
    nbr_ref,
    rel_ref,
    send_ref,
    act_ref,
    ct_ref,
    out_ref,
    gw_ref,
    halo_s,
    halo_r,
    hid_s,
    hid_r,
    dh_s,
    dh_r,
    back_s,
    back_r,
    zt,
    zt_p,
    dt,
    dt_p,
    gx_s,
    gx_r,
    gy_s,
    gy_r,
    gz_s,
    gz_r,
    ga_r,
    q_ref,
    ktab,
    vtab,
    cmat,
    attn,
    agg_ref,
    dq_ref,
    dkv,
    tp,
    halo_sem,
    hid_sem,
    dh_sem,
    back_sem,
    pair_sem,
    gx_sem,
    gy_sem,
    gz_sem,
    ga_sem,
):
    nz, nx, ny = sizes
    n_dom, n_snap = nz * nx, 2 * ny
    rows, width = x_ref.shape
    halo = n_dom * 8
    table = rows + halo
    block = rows // n_snap
    cols = 3 * width // nx
    scale = (width // HEADS) ** -0.5

    me_d = lax.axis_index("dom")
    me_s = lax.axis_index("snap")
    me_z, me_x = me_d // nx, lax.rem(me_d, nx)
    me_y, me_c = me_s // 2, lax.rem(me_s, 2)
    partner = {"snap": me_s + 1 - 2 * me_c}

    barrier = pltpu.get_barrier_semaphore()

    def greet_dom(step, carry):
        pl.semaphore_signal(
            barrier, inc=1, device_id={"dom": lax.rem(me_d + step, n_dom)}, device_id_type=MESH
        )
        return carry

    def greet_snap(step, carry):
        pl.semaphore_signal(
            barrier, inc=1, device_id={"snap": lax.rem(me_s + step, n_snap)}, device_id_type=MESH
        )
        return carry

    lax.fori_loop(1, n_dom, greet_dom, 0)
    lax.fori_loop(1, n_snap, greet_snap, 0)

    halo_x = Exchange(
        n_dom, me_d, lambda p: {"dom": p}, lambda p: halo_s.at[p], halo_r, halo_sem
    )
    hid_x = Exchange(n_snap, me_s, lambda p: {"snap": p}, lambda p: hid_s.at[p], hid_r, hid_sem)
    dh_x = Exchange(n_snap, me_s, lambda p: {"snap": p}, lambda p: dh_s.at[p], dh_r, dh_sem)
    back_x = Exchange(
        n_dom, me_d, lambda p: {"dom": p}, lambda p: back_s.at[p], back_r, back_sem
    )
    gx_x = Exchange(
        nx, me_x, lambda p: {"dom": me_z * nx + p}, lambda p: gx_s.at[p], gx_r, gx_sem
    )
    gy_x = Exchange(
        ny, me_y, lambda p: {"snap": p * 2 + me_c}, lambda p: gy_s.at[p], gy_r, gy_sem
    )
    gz_x = Exchange(nz, me_z, lambda p: {"dom": p * nx + me_x}, lambda p: gz_s, gz_r, gz_sem)
    ga_x = Exchange(
        nx, me_x, lambda p: {"dom": me_z * nx + p}, lambda p: ga_r.at[me_x], ga_r, ga_sem
    )

    send_f = send_ref[...].astype(F32).astype(BF)
    spread = (lax.rem(iota((8, halo), 1), 8) == iota((8, halo), 0)).astype(F32).astype(BF)
    wide = mm(send_f, spread)
    picked = jnp.where(iota((n_dom, halo), 1) // 8 == iota((n_dom, halo), 0), wide, 0.0)
    send_row = jnp.sum(picked, axis=0, keepdims=True)
    pick_t = (iota((rows, halo), 0).astype(F32) == send_row).astype(F32)
    x_val = x_ref[...]
    tiles = mm(pick_t.T.astype(BF), x_val)
    halo_s[...] = tiles.reshape(n_dom, 8, width).astype(BF)

    pl.semaphore_wait(barrier, n_dom + n_snap - 2)
    halo_x.start()
    halo_r[me_d] = halo_s[me_d]

    own = mm(x_val, ws_ref[...]).astype(BF)
    q_ref[...] = own[:, :width]
    ktab[0:rows, :] = own[:, width : 2 * width]
    vtab[0:rows, :] = own[:, 2 * width :]

    nbr = nbr_ref[...]
    place = 1 << (4 * rel_ref[...])
    lane_t = iota((rows, table), 1)
    packed = jnp.zeros((rows, table), jnp.int32)
    for k in range(nbr.shape[1]):
        packed += jnp.where(lane_t == nbr[:, k : k + 1], place[:, k : k + 1], 0)
    counts = [((packed >> (4 * r)) & 15).astype(F32) for r in range(4)]
    eb = jnp.exp(rb_ref[...])
    for h in range(HEADS):
        total = counts[0] * eb[0:1, h : h + 1]
        for r in range(1, 4):
            total += counts[r] * eb[r : r + 1, h : h + 1]
        cmat[h] = total

    row_i = iota((rows, rows), 0)
    col_i = iota((rows, rows), 1)
    act_f = act_ref[...].astype(F32).astype(BF)
    over = (lax.rem(iota((block, rows), 1), block) == iota((block, rows), 0)).astype(F32)
    act_w = mm(act_f, over.astype(BF))
    act_row = jnp.sum(
        jnp.where(iota((n_snap, rows), 1) // block == iota((n_snap, rows), 0), act_w, 0.0),
        axis=0,
        keepdims=True,
    )
    same = lax.rem(row_i, block) == lax.rem(col_i, block)
    earlier = jnp.where(col_i // block <= row_i // block, act_row, 0.0)
    allowed = jnp.where(row_i == col_i, 1.0, jnp.where(same, earlier, 0.0))
    step_1h = (iota((rows, n_snap), 0) // block == iota((rows, n_snap), 1)).astype(F32)
    pos_rows = mm(step_1h.astype(BF), pos_ref[...])

    halo_x.wait_recv()
    halo_rows = halo_r[...].astype(F32).reshape(halo, width).astype(BF)
    ktab[rows:, :] = mm(halo_rows, ws_ref[:, width : 2 * width]).astype(BF)
    vtab[rows:, :] = mm(halo_rows, ws_ref[:, 2 * width :]).astype(BF)

    half = iota((rows, 128), 1) < 64
    halves = (half, jnp.logical_not(half))
    pairs = HEADS // 2

    for p in range(pairs):
        at = slice(128 * p, 128 * p + 128)
        q_p, k_p, v_p = q_ref[:, at], ktab[:, at], vtab[:, at]
        outs = []
        for s in range(2):
            score = mm_nt(where_bf(halves[s], q_p), k_p) * scale
            c = cmat[2 * p + s]
            score = jnp.where(c > 0, score, -1e30)
            e = jnp.exp(score - jnp.max(score, axis=1, keepdims=True)) * c
            w = e / jnp.sum(e, axis=1, keepdims=True)
            attn[2 * p + s] = w
            outs.append(mm(w.astype(BF), v_p))
        agg_ref[:, at] = jnp.where(half, outs[0], outs[1])
    agg = agg_ref[...]
    hidden = x_val.astype(F32) + jnp.where(agg > 0, agg, jnp.exp(jnp.minimum(agg, 0.0)) - 1.0)
    hid_s[...] = hidden.reshape(n_snap, block, width).astype(BF)
    hid_x.start()
    hid_r[me_s] = hid_s[me_s]

    ct_f = ct_ref[...].astype(F32).reshape(rows, width)
    ct = ct_f.astype(BF)
    hid_x.wait_recv()
    z_f = hid_r[...].astype(F32).reshape(rows, width).astype(F32) + pos_rows
    z = z_f.astype(BF)
    tp[...] = mm(z, wt_ref[...]).astype(BF)
    zt[...] = z_f.T.astype(BF).reshape(ny, 2, width // n_snap, rows)
    for p in range(pairs):
        at = slice(128 * p, 128 * p + 128)
        q_p = tp[:, 128 * p : 128 * p + 128]
        k_p = tp[:, width + 128 * p : width + 128 * p + 128]
        v_p = tp[:, 2 * width + 128 * p : 2 * width + 128 * p + 128]
        ct_p = ct[:, at]
        parts = []
        for s in range(2):
            score = mm_nt(where_bf(halves[s], q_p), k_p) * scale
            score = jnp.where(allowed > 0, score, -1e30)
            e = jnp.exp(score - jnp.max(score, axis=1, keepdims=True))
            w = e / jnp.sum(e, axis=1, keepdims=True)
            d_w = mm_nt(where_bf(halves[s], ct_p), v_p)
            t = w * d_w
            d_s = (t - w * jnp.sum(t, axis=1, keepdims=True)) * scale
            parts.append(
                (mm(d_s.astype(BF), k_p), mm(d_s.T.astype(BF), q_p), mm(w.T.astype(BF), ct_p))
            )
        for i in range(3):
            dt[:, width * i + 128 * p : width * i + 128 * p + 128] = jnp.where(
                half, parts[0][i], parts[1][i]
            ).astype(BF)

    pair_z = copy_to(
        zt.at[:, 1 - me_c], zt_p, pair_sem.at[0, 0], pair_sem.at[1, 0], partner
    )
    pair_d = copy_to(dt, dt_p, pair_sem.at[0, 1], pair_sem.at[1, 1], partner)
    pair_z.start()
    pair_d.start()

    d_z = ct_f + mm_nt(dt[...], wt_ref[...])
    dh_s[...] = d_z.reshape(n_snap, block, width).astype(BF)
    dh_x.start()
    dh_r[me_s] = dh_s[me_s]

    pair_z.wait_recv()
    pair_d.wait_recv()
    z_both = jnp.concatenate(
        [zt[:, me_c].reshape(width // 2, rows), zt_p[...].reshape(width // 2, rows)], axis=1
    )
    for i in range(nx):
        cut = slice(cols * i, cols * i + cols)
        d_both = jnp.concatenate([dt[:, cut], dt_p[:, cut]], axis=0)
        gx_s[i] = mm(z_both, d_both).astype(BF)
    gx_x.start()

    dh_x.wait_recv()
    dh_f = dh_r[...].astype(F32).reshape(rows, width)
    agg = agg_ref[...]
    d_agg = dh_f * jnp.where(agg > 0, 1.0, jnp.exp(jnp.minimum(agg, 0.0)))
    d_agg = d_agg.astype(BF)
    half_t = iota((table, 128), 1) < 64
    for p in range(pairs):
        at = slice(128 * p, 128 * p + 128)
        q_p, k_p, v_p = q_ref[:, at], ktab[:, at], vtab[:, at]
        da_p = d_agg[:, at]
        parts = []
        for s in range(2):
            w = attn[2 * p + s]
            d_w = mm_nt(where_bf(halves[s], da_p), v_p)
            t = w * d_w
            d_s = (t - w * jnp.sum(t, axis=1, keepdims=True)) * scale
            parts.append(
                (mm(d_s.astype(BF), k_p), mm(d_s.T.astype(BF), q_p), mm(w.T.astype(BF), da_p))
            )
        dq_ref[:, at] = jnp.where(half, parts[0][0], parts[1][0]).astype(BF)
        dkv[:, at] = jnp.where(half_t, parts[0][1], parts[1][1]).astype(BF)
        dkv[:, width + 128 * p : width + 128 * p + 128] = jnp.where(
            half_t, parts[0][2], parts[1][2]
        ).astype(BF)

    d_halo = mm_nt(dkv[rows:, :], ws_ref[:, width:])
    back_s[...] = d_halo.reshape(n_dom, 8, width).astype(BF)
    back_x.start()
    back_r[me_d] = back_s[me_d]

    gx_x.wait_recv()
    gx_r[me_x] = gx_s[me_x]
    total = gx_r[0].astype(F32)
    for i in range(1, nx):
        total += gx_r[i].astype(F32)
    gy_s[...] = total.astype(BF).reshape(ny, width // n_snap, cols)
    gy_x.start()

    d_own = dh_f + mm_nt(dq_ref[...], ws_ref[:, :width]) + mm_nt(dkv[0:rows, :], ws_ref[:, width:])

    gy_x.wait_recv()
    gy_r[me_y] = gy_s[me_y]
    total = gy_r[0].astype(F32)
    for i in range(1, ny):
        total += gy_r[i].astype(F32)
    gz_s[...] = total.astype(BF)
    gz_x.start()
    gz_r[me_z] = gz_s[...]

    back_x.wait_recv()
    came = back_r[...].astype(F32).reshape(halo, width).astype(BF)
    out_ref[...] = (d_own + mm(pick_t.astype(BF), came)).astype(BF)

    gz_x.wait_recv()
    total = gz_r[0].astype(F32)
    for i in range(1, nz):
        total += gz_r[i].astype(F32)
    ga_r[me_x] = total.astype(BF)
    ga_x.start()
    ga_x.wait_recv()
    for i in range(nx):
        gw_ref[:, cols * i : cols * i + cols] = ga_r[i].astype(F32)

    for exchange in (halo_x, hid_x, dh_x, back_x, gx_x, gy_x, gz_x, ga_x):
        exchange.wait_send()
    pair_z.wait_send()
    pair_d.wait_send()


def per_device(
    feat, w_struct, w_temp, pos_embed, rel_bias, nbr, rel_type, send_idx, active, cotangent
):
    x = feat[0]
    rows, width = x.shape
    n_dom, n_snap = lax.axis_size("dom"), lax.axis_size("snap")
    nz, nx = GRID[n_dom]
    ny = n_snap // 2
    halo = n_dom * 8
    table = rows + halo
    block = rows // n_snap
    cols = 3 * width // nx
    wrows = width // n_snap
    vm = pltpu.VMEM
    dma = pltpu.SemaphoreType.DMA
    scratch = [
        vm((n_dom, 8, width), BF),
        vm((n_dom, 8, width), BF),
        vm((n_snap, block, width), BF),
        vm((n_snap, block, width), BF),
        vm((n_snap, block, width), BF),
        vm((n_snap, block, width), BF),
        vm((n_dom, 8, width), BF),
        vm((n_dom, 8, width), BF),
        vm((ny, 2, wrows, rows), BF),
        vm((ny, wrows, rows), BF),
        vm((rows, 3 * width), BF),
        vm((rows, 3 * width), BF),
        vm((nx, width // 2, cols), BF),
        vm((nx, width // 2, cols), BF),
        vm((ny, wrows, cols), BF),
        vm((ny, wrows, cols), BF),
        vm((wrows, cols), BF),
        vm((nz, wrows, cols), BF),
        vm((nx, wrows, cols), BF),
        vm((rows, width), BF),
        vm((table, width), BF),
        vm((table, width), BF),
        vm((HEADS, rows, table), F32),
        vm((HEADS, rows, table), F32),
        vm((rows, width), F32),
        vm((rows, width), BF),
        vm((table, 2 * width), BF),
        vm((rows, 3 * width), BF),
        dma((2, n_dom)),
        dma((2, n_snap)),
        dma((2, n_snap)),
        dma((2, n_dom)),
        dma((2, 2)),
        dma((2, nx)),
        dma((2, ny)),
        dma((2, nz)),
        dma((2, nx)),
    ]
    grad, gw = pl.pallas_call(
        functools.partial(kernel, (nz, nx, ny)),
        out_shape=(
            jax.ShapeDtypeStruct((rows, width), BF),
            jax.ShapeDtypeStruct((wrows, 3 * width), F32),
        ),
        in_specs=[pl.BlockSpec(memory_space=pltpu.VMEM)] * 10,
        out_specs=(pl.BlockSpec(memory_space=pltpu.VMEM),) * 2,
        scratch_shapes=scratch,
        compiler_params=pltpu.CompilerParams(collective_id=0, has_side_effects=True),
        name="step",
    )(
        x,
        w_struct,
        w_temp,
        pos_embed,
        rel_bias,
        nbr[0],
        rel_type[0],
        send_idx[0, 0],
        active,
        cotangent,
    )
    return (grad[None], gw)


def solution(mesh):
    return jax.shard_map(
        per_device,
        mesh=mesh,
        in_specs=(
            P("snap", "dom", None),
            P(),
            P(),
            P(),
            P(),
            P("snap", "dom", None),
            P("snap", "dom", None),
            P("snap", "dom", None, None),
            P(None, ("dom", "snap")),
            P(None, ("dom", "snap"), None),
        ),
        out_specs=(P("snap", "dom", None), P("snap", None)),
        check_vma=False,
    )
```

```python
import functools

import jax
import jax.numpy as jnp
from jax import lax
from jax.experimental import pallas as pl
from jax.experimental.pallas import tpu as pltpu
from jax.sharding import PartitionSpec as P

HEADS = 8
MESH = pl.DeviceIdType.MESH
BF = jnp.bfloat16
F32 = jnp.float32
GRID = {32: (8, 4), 4: (2, 2), 8: (2, 4)}


def mm(a, b):
    return jnp.dot(a, b, preferred_element_type=F32)


def mm_nt(a, b):
    return lax.dot_general(a, b, (((1,), (1,)), ((), ())), preferred_element_type=F32)


def mm_tn(a, b):
    return lax.dot_general(a, b, (((0,), (0,)), ((), ())), preferred_element_type=F32)


def iota(shape, axis):
    return lax.broadcasted_iota(jnp.int32, shape, axis)


def where_bf(mask, value):
    return jnp.where(mask, value, jnp.zeros_like(value))


def copy_to(src, dst, send_sem, recv_sem, device):
    return pltpu.make_async_remote_copy(
        src_ref=src,
        dst_ref=dst,
        send_sem=send_sem,
        recv_sem=recv_sem,
        device_id=device,
        device_id_type=MESH,
    )


class Exchange:
    def __init__(self, count, me, device_of, src, dst, sems):
        self.count, self.me, self.device_of = count, me, device_of
        self.src, self.dst, self.send, self.recv = src, dst, sems.at[0], sems.at[1]

    def each(self, act):
        def body(step, carry):
            near = (step + 1) // 2
            shift = near + (step + 1) % 2 * (self.count - 2 * near)
            act(lax.rem(self.me + shift, self.count))
            return carry

        lax.fori_loop(1, self.count, body, 0)

    def start(self):
        self.each(
            lambda peer: copy_to(
                self.src(peer),
                self.dst.at[self.me],
                self.send.at[peer],
                self.recv.at[self.me],
                self.device_of(peer),
            ).start()
        )

    def wait_recv(self):
        self.each(
            lambda peer: copy_to(
                self.src(peer),
                self.dst.at[peer],
                self.send.at[peer],
                self.recv.at[peer],
                self.device_of(peer),
            ).wait_recv()
        )

    def wait_send(self):
        self.each(
            lambda peer: copy_to(
                self.src(peer),
                self.dst.at[peer],
                self.send.at[peer],
                self.recv.at[peer],
                self.device_of(peer),
            ).wait_send()
        )


def kernel(
    sizes,
    x_hbm,
    ws_hbm,
    wt_hbm,
    pos_hbm,
    rb_hbm,
    nbr_hbm,
    rel_hbm,
    send_hbm,
    act_hbm,
    ct_hbm,
    out_hbm,
    gw_hbm,
    x_ref,
    ws_ref,
    wt_ref,
    pos_ref,
    rb_ref,
    nbr_ref,
    rel_ref,
    send_ref,
    act_ref,
    ct_ref,
    in_sem,
    out_ref,
    gw_ref,
    out_sem,
    halo_s,
    halo_r,
    hid_s,
    hid_r,
    dh_s,
    dh_r,
    back_s,
    back_r,
    zt,
    zt_p,
    dt,
    dt_p,
    gx_s,
    gx_r,
    gx_v,
    xy_s,
    xy_r,
    xz_s,
    xz_r,
    xa_r,
    zz_s,
    zz_r,
    zy_s,
    zy_r,
    zx_r,
    za_r,
    qst,
    ktab,
    vtab,
    wvt,
    vt,
    ktt,
    cmat,
    attn,
    attn_b,
    d_att,
    d_sc,
    das,
    agg_t,
    slope,
    dkv,
    allow,
    pos_rows,
    cts,
    tp,
    tqs,
    t_s,
    t_d,
    t_w,
    t_b,
    halo_sem,
    hid_sem,
    dh_sem,
    back_sem,
    pair_sem,
    gx_sem,
    xy_sem,
    xz_sem,
    xa_sem,
    zz_sem,
    zy_sem,
    zx_sem,
    za_sem,
):
    nz, nx, ny = sizes
    n_dom, n_snap = nz * nx, 2 * ny
    rows, width = x_ref.shape
    halo = n_dom * 8
    table = rows + halo
    block = rows // n_snap
    cols = 2 * width // nx
    wrows = width // n_snap
    xrows, zc = wrows // (nz // 2), min(4, nz)
    zrows, zcols = wrows // (nz // zc), width // zc
    scale = (width // HEADS) ** -0.5
    scale_bf = jnp.asarray(scale, BF)
    pairs = HEADS // 2

    loads = {
        "send": (send_hbm, send_ref),
        "x": (x_hbm, x_ref),
        "ws": (ws_hbm, ws_ref),
        "nbr": (nbr_hbm, nbr_ref),
        "rel": (rel_hbm, rel_ref),
        "rb": (rb_hbm, rb_ref),
        "act": (act_hbm, act_ref),
        "pos": (pos_hbm, pos_ref),
        "ct": (ct_hbm, ct_ref),
        "wt": (wt_hbm, wt_ref),
    }
    order = list(loads)

    def input_copy(name):
        return pltpu.make_async_copy(*loads[name], in_sem.at[order.index(name)])

    def arrive(name, load=True):
        input_copy(name).wait()
        return loads[name][1][...] if load else None

    for name in order:
        input_copy(name).start()

    me_d = lax.axis_index("dom")
    me_s = lax.axis_index("snap")
    me_z, me_x = me_d // nx, lax.rem(me_d, nx)
    me_y, me_c = me_s // 2, lax.rem(me_s, 2)
    partner = {"snap": me_s + 1 - 2 * me_c}

    barrier = pltpu.get_barrier_semaphore()

    def greet_dom(step, carry):
        pl.semaphore_signal(
            barrier, inc=1, device_id={"dom": lax.rem(me_d + step, n_dom)}, device_id_type=MESH
        )
        return carry

    def greet_snap(step, carry):
        pl.semaphore_signal(
            barrier, inc=1, device_id={"snap": lax.rem(me_s + step, n_snap)}, device_id_type=MESH
        )
        return carry

    lax.fori_loop(1, n_dom, greet_dom, 0)
    lax.fori_loop(1, n_snap, greet_snap, 0)

    halo_x = Exchange(
        n_dom, me_d, lambda p: {"dom": p}, lambda p: halo_s.at[p], halo_r, halo_sem
    )
    hid_x = Exchange(n_snap, me_s, lambda p: {"snap": p}, lambda p: hid_s.at[p], hid_r, hid_sem)
    dh_x = Exchange(n_snap, me_s, lambda p: {"snap": p}, lambda p: dh_s.at[p], dh_r, dh_sem)
    back_x = Exchange(
        n_dom, me_d, lambda p: {"dom": p}, lambda p: back_s.at[p], back_r, back_sem
    )
    py_x = Exchange(
        ny, me_y, lambda p: {"snap": p * 2 + me_c}, lambda p: xy_s.at[p], xy_r, xy_sem
    )
    pz_x = Exchange(nz, me_z, lambda p: {"dom": p * nx + me_x}, lambda p: xz_s.at[p], xz_r, xz_sem)
    pa_x = Exchange(n_dom, me_d, lambda p: {"dom": p}, lambda p: xa_r.at[me_d], xa_r, xa_sem)
    qz_x = Exchange(nz, me_z, lambda p: {"dom": p * nx + me_x}, lambda p: zz_s.at[p], zz_r, zz_sem)
    qy_x = Exchange(
        ny, me_y, lambda p: {"snap": p * 2 + me_c}, lambda p: zy_s.at[p], zy_r, zy_sem
    )
    qx_x = Exchange(
        nx, me_x, lambda p: {"dom": me_z * nx + p}, lambda p: zx_r.at[me_x], zx_r, zx_sem
    )
    qa_x = Exchange(
        nz, me_z, lambda p: {"dom": p * nx + me_x}, lambda p: za_r.at[me_z], za_r, za_sem
    )
    right, left = lax.rem(me_x + 1, nx), lax.rem(me_x + nx - 1, nx)
    to_right, to_left = {"dom": me_z * nx + right}, {"dom": me_z * nx + left}
    mid = width // 4
    top, low = pl.ds(0, mid), pl.ds(mid, mid)

    def neighbour(src, dst, slot, device):
        return copy_to(src, dst, gx_sem.at[0, slot], gx_sem.at[1, slot], device)

    if nx == 4:
        across = lax.rem(me_x + 2, nx)
        hops = [
            neighbour(gx_s.at[across, top], gx_v.at[0], 0, to_right),
            neighbour(gx_s.at[across, low], gx_v.at[1], 1, to_left),
            neighbour(gx_s.at[right, low], gx_r.at[0, low], 2, to_right),
            neighbour(gx_s.at[left, top], gx_r.at[1, top], 3, to_left),
            neighbour(gx_v.at[2], gx_r.at[0, top], 4, to_right),
            neighbour(gx_v.at[3], gx_r.at[1, low], 5, to_left),
        ]
    else:
        hops = [neighbour(gx_s.at[right], gx_r.at[0], 0, to_right)]

    send_f = arrive("send").astype(F32).astype(BF)
    spread = (iota((n_dom, halo), 1) // 8 == iota((n_dom, halo), 0)).astype(F32).astype(BF)
    wide = mm(send_f, spread)
    picked = jnp.where(lax.rem(iota((8, halo), 1), 8) == iota((8, halo), 0), wide, 0.0)
    send_row = jnp.sum(picked, axis=0, keepdims=True)
    pick_t = (iota((rows, halo), 0).astype(F32) == send_row).astype(F32)
    pick = pick_t.T.astype(BF)
    x_val = arrive("x")
    tiles = mm(pick, x_val)
    halo_s[...] = tiles.reshape(n_dom, 8, width).astype(BF)

    pl.semaphore_wait(barrier, n_dom + n_snap - 2)
    halo_x.start()
    halo_r[me_d] = halo_s[me_d]

    half = iota((rows, 128), 1) < 64

    def stack(value):
        zero = jnp.zeros_like(value)
        return jnp.concatenate(
            [jnp.where(half, value, zero), jnp.where(half, zero, value)], axis=0
        )

    w_v = pl.ds(2 * width, width)
    arrive("ws", load=False)
    own = mm(x_val, ws_ref[...]).astype(BF)
    ktab[0:rows, :] = own[:, width : 2 * width]
    vtab[0:rows, :] = own[:, 2 * width :]
    for p in range(pairs):
        qst[p] = stack(own[:, 128 * p : 128 * p + 128] * scale_bf)
    wvt[...] = ws_ref[:, w_v].T
    vt[:, 0:rows] = mm_nt(wvt[...], x_val).astype(BF)

    nbr = arrive("nbr").astype(F32)
    slots = nbr.shape[0]
    place = (1 << (4 * arrive("rel"))).astype(F32)
    row_t = iota((table, rows), 0).astype(F32)
    packed = jnp.zeros((table, rows), F32)
    for k in range(slots):
        packed += jnp.where(row_t == nbr[k : k + 1, :], place[k : k + 1, :], 0.0)
    packed = packed.astype(jnp.int32)
    counts = [((packed >> (4 * r)) & 15).astype(F32) for r in range(4)]
    eb = jnp.exp(arrive("rb"))
    for h in range(HEADS):
        total = counts[0] * eb[0:1, h : h + 1]
        for r in range(1, 4):
            total += counts[r] * eb[r : r + 1, h : h + 1]
        cmat[h // 2, :, (h % 2) * rows : (h % 2) * rows + rows] = total

    row_i = iota((rows, rows), 0)
    col_i = iota((rows, rows), 1)
    act_f = arrive("act").astype(F32).astype(BF)
    over = (iota((n_snap, rows), 1) // block == iota((n_snap, rows), 0)).astype(F32)
    act_w = mm(act_f, over.astype(BF))
    act_own = lax.rem(iota((block, rows), 1), block) == iota((block, rows), 0)
    act_row = jnp.sum(jnp.where(act_own, act_w, 0.0), axis=0, keepdims=True)
    same = lax.rem(row_i, block) == lax.rem(col_i, block)
    earlier = jnp.where(col_i // block <= row_i // block, act_row, 0.0)
    allowed = jnp.where(row_i == col_i, 1.0, jnp.where(same, earlier, 0.0)).T
    allow[:, 0:rows] = allowed
    allow[:, rows:] = allowed
    step_1h = (iota((rows, n_snap), 0) // block == iota((rows, n_snap), 1)).astype(F32)
    pos_rows[...] = mm(step_1h.astype(BF), arrive("pos"))
    ct_f = arrive("ct").astype(F32).reshape(rows, width)
    ct = ct_f.astype(BF)
    for p in range(pairs):
        cts[p] = stack(ct[:, 128 * p : 128 * p + 128])

    halo_x.wait_recv()
    halo_rows = halo_r[...].astype(F32).reshape(halo, width).astype(BF)
    ktab[rows:, :] = mm(halo_rows, ws_ref[:, width : 2 * width]).astype(BF)
    vt[:, rows:] = mm_nt(wvt[...], halo_rows).astype(BF)

    for p in range(pairs):
        attn[p] = mm_nt(ktab[:, 128 * p : 128 * p + 128], qst[p])
    for p in range(pairs):
        c = cmat[p]
        score = jnp.where(c > 0, attn[p], -1e30)
        e = jnp.exp(score - jnp.max(score, axis=0, keepdims=True)) * c
        w = e * (1.0 / jnp.sum(e, axis=0, keepdims=True))
        attn[p] = w
        attn_b[p] = w.astype(BF)
    for p in range(pairs):
        o = mm(vt[128 * p : 128 * p + 128, :], attn_b[p])
        agg_t[128 * p : 128 * p + 64, :] = o[0:64, 0:rows]
        agg_t[128 * p + 64 : 128 * p + 128, :] = o[64:128, rows:]
    agg = agg_t[...].T
    hidden = x_val.astype(F32) + jnp.where(agg > 0, agg, jnp.exp(jnp.minimum(agg, 0.0)) - 1.0)
    hid_s[...] = hidden.reshape(n_snap, block, width).astype(BF)
    hid_x.start()
    hid_r[me_s] = hid_s[me_s]
    slope[...] = jnp.where(agg > 0, 1.0, jnp.exp(jnp.minimum(agg, 0.0)))
    vtab[rows:, :] = mm(halo_rows, ws_ref[:, w_v]).astype(BF)
    ktt[...] = ktab[...].T
    arrive("wt", load=False)
    halo_x.wait_send()

    hid_x.wait_recv()
    z_f = hid_r[...].astype(F32).reshape(rows, width) + pos_rows[...]
    z = z_f.astype(BF)
    tp[...] = mm(z, wt_ref[...]).astype(BF)
    zt[...] = z_f.T.astype(BF).reshape(ny, 2, width // n_snap, rows)
    for p in range(pairs):
        tqs[p] = stack(tp[:, 128 * p : 128 * p + 128] * scale_bf)
        t_s[p] = mm_nt(tp[:, width + 128 * p : width + 128 * p + 128], tqs[p])
        t_d[p] = mm_nt(tp[:, 2 * width + 128 * p : 2 * width + 128 * p + 128], cts[p])
    for p in range(pairs):
        score = jnp.where(allow[...] > 0, t_s[p], -1e30)
        e = jnp.exp(score - jnp.max(score, axis=0, keepdims=True))
        w = e * (1.0 / jnp.sum(e, axis=0, keepdims=True))
        t = w * t_d[p]
        t_w[p] = w.astype(BF)
        t_b[p] = (t - w * jnp.sum(t, axis=0, keepdims=True)).astype(BF)
    for p in range(pairs):
        at = 128 * p
        dq = mm_tn(t_b[p], tp[:, width + at : width + at + 128]) * scale
        dt[:, at : at + 128] = jnp.where(half, dq[0:rows], dq[rows:]).astype(BF)
        dt[:, width + at : width + at + 128] = mm(t_b[p], tqs[p]).astype(BF)
        dt[:, 2 * width + at : 2 * width + at + 128] = mm(t_w[p], cts[p]).astype(BF)

    pair_z = copy_to(
        zt.at[:, 1 - me_c], zt_p, pair_sem.at[0, 0], pair_sem.at[1, 0], partner
    )
    pair_d = copy_to(dt, dt_p, pair_sem.at[0, 1], pair_sem.at[1, 1], partner)
    pair_z.start()
    pair_d.start()

    d_z = ct_f + mm_nt(dt[...], wt_ref[...])
    dh_s[...] = d_z.reshape(n_snap, block, width).astype(BF)
    dh_x.start()
    dh_r[me_s] = dh_s[me_s]

    pair_z.wait_recv()
    pair_d.wait_recv()
    z_both = jnp.concatenate(
        [zt[:, me_c].reshape(width // 2, rows), zt_p[...].reshape(width // 2, rows)], axis=1
    )
    d_both = jnp.concatenate([dt[:, 0 : 2 * width], dt_p[:, 0 : 2 * width]], axis=0)
    for i in range(nx):
        gx_s[i] = mm(z_both, d_both[:, cols * i : cols * i + cols]).astype(BF)
    d_both = jnp.concatenate([dt[:, 2 * width :], dt_p[:, 2 * width :]], axis=0)
    product = mm(z_both, d_both).reshape(ny, wrows, width)
    for i in range(nz):
        r, c = i // zc * zrows, i % zc * zcols
        zz_s[i] = product[:, r : r + zrows, c : c + zcols].astype(BF)
    for hop in hops[0:4]:
        hop.start()
    qz_x.start()
    zz_r[me_z] = zz_s[me_z]
    if nx == 4:
        hops[0].wait_recv()
        hops[1].wait_recv()
        gx_v[2] = (gx_s[right, top].astype(F32) + gx_v[0].astype(F32)).astype(BF)
        gx_v[3] = (gx_s[left, low].astype(F32) + gx_v[1].astype(F32)).astype(BF)
        hops[4].start()
        hops[5].start()

    hid_x.wait_send()
    dh_x.wait_recv()
    dh_f = dh_r[...].astype(F32).reshape(rows, width)
    d_agg = (dh_f * slope[...]).astype(BF)
    for p in range(pairs):
        das[p] = stack(d_agg[:, 128 * p : 128 * p + 128])
        d_att[p] = mm_nt(vtab[:, 128 * p : 128 * p + 128], das[p])
    for p in range(pairs):
        w = attn[p]
        t = w * d_att[p]
        d_sc[p] = (t - w * jnp.sum(t, axis=0, keepdims=True)).astype(BF)
    for p in range(pairs):
        at = 128 * p
        dkv[rows:, at : at + 128] = mm(d_sc[p, rows:, :], qst[p]).astype(BF)
        dkv[rows:, width + at : width + at + 128] = mm(attn_b[p, rows:, :], das[p]).astype(BF)

    d_halo = mm_nt(dkv[rows:, :], ws_ref[:, width:])
    back_s[...] = d_halo.reshape(n_dom, 8, width).astype(BF)
    back_x.start()
    back_r[me_d] = back_s[me_d]

    for hop in hops[2:] if nx == 4 else hops:
        hop.wait_recv()
    total = gx_s[me_x].astype(F32) + gx_r[0].astype(F32)
    if nx == 4:
        total += gx_r[1].astype(F32)
    xy_s[...] = total.astype(BF).reshape(ny, wrows, cols)
    py_x.start()
    xy_r[me_y] = xy_s[me_y]

    for p in range(pairs):
        at = 128 * p
        dkv[0:rows, at : at + 128] = mm(d_sc[p, 0:rows, :], qst[p]).astype(BF)
        dkv[0:rows, width + at : width + at + 128] = mm(attn_b[p, 0:rows, :], das[p]).astype(BF)
        o = mm(ktt[at : at + 128, :], d_sc[p]) * scale
        agg_t[at : at + 64, :] = o[0:64, 0:rows]
        agg_t[at + 64 : at + 128, :] = o[64:128, rows:]
    dq = agg_t[...].T.astype(BF)
    d_own = dh_f + mm_nt(dq, ws_ref[:, :width]) + mm_nt(dkv[0:rows, :], ws_ref[:, width:])
    dh_x.wait_send()
    pair_z.wait_send()
    pair_d.wait_send()
    for hop in hops:
        hop.wait_send()

    def total_of(ref, count):
        total = ref[0].astype(F32)
        for i in range(1, count):
            total += ref[i].astype(F32)
        return total

    qz_x.wait_recv()
    zy_s[...] = total_of(zz_r, nz).astype(BF)
    qy_x.start()
    zy_r[me_y] = zy_s[me_y]

    py_x.wait_recv()
    total = total_of(xy_r, ny)
    for i in range(nz):
        r, c = i // 2 * xrows, i % 2 * 128
        xz_s[i] = total[r : r + xrows, c : c + 128].astype(BF)
    pz_x.start()
    xz_r[me_z] = xz_s[me_z]
    qz_x.wait_send()
    py_x.wait_send()

    qy_x.wait_recv()
    zx_r[me_x] = total_of(zy_r, ny).astype(BF)
    qx_x.start()
    qy_x.wait_send()

    back_x.wait_recv()
    came = back_r[...].astype(F32).reshape(halo, width).astype(BF)
    out_ref[...] = (d_own + mm(pick_t.astype(BF), came)).astype(BF)
    save_out = pltpu.make_async_copy(out_ref, out_hbm, out_sem.at[0])
    save_out.start()

    pz_x.wait_recv()
    xa_r[me_d] = total_of(xz_r, nz).astype(BF)
    pa_x.start()
    qx_x.wait_recv()
    za_r[me_z] = total_of(zx_r, nx).astype(BF)
    qa_x.start()
    back_x.wait_send()
    pz_x.wait_send()
    qx_x.wait_send()
    qa_x.wait_recv()
    for i in range(nz):
        r, c = i // zc * zrows, 2 * width + i % zc * zcols
        gw_ref[r : r + zrows, c : c + zcols] = za_r[i].astype(F32)
    pa_x.wait_recv()
    for i in range(n_dom):
        r, c = i // nx // 2 * xrows, i % nx * cols + i // nx % 2 * 128
        gw_ref[r : r + xrows, c : c + 128] = xa_r[i].astype(F32)
    save_gw = pltpu.make_async_copy(gw_ref, gw_hbm, out_sem.at[1])
    save_gw.start()
    pa_x.wait_send()
    qa_x.wait_send()
    save_out.wait()
    save_gw.wait()


def emit(grad_ref, gw_ref, grad_out, gw_out):
    grad_out[...] = grad_ref[...]
    gw_out[...] = gw_ref[...]


def per_device(
    feat, w_struct, w_temp, pos_embed, rel_bias, nbr, rel_type, send_idx, active, cotangent
):
    x = feat[0]
    rows, width = x.shape
    n_dom, n_snap = lax.axis_size("dom"), lax.axis_size("snap")
    nz, nx = GRID[n_dom]
    ny = n_snap // 2
    halo = n_dom * 8
    table = rows + halo
    block = rows // n_snap
    cols = 2 * width // nx
    wrows = width // n_snap
    xrows, zc = wrows // (nz // 2), min(4, nz)
    zrows, zcols = wrows // (nz // zc), width // zc
    vm = pltpu.VMEM
    dma = pltpu.SemaphoreType.DMA
    arrays = (
        x,
        w_struct,
        w_temp,
        pos_embed,
        rel_bias,
        nbr[0].T,
        rel_type[0].T,
        send_idx[0, 0].T,
        active.T,
        cotangent,
    )
    pairs = HEADS // 2
    scratch = [vm(a.shape, a.dtype) for a in arrays] + [
        dma((len(arrays),)),
        vm((rows, width), BF),
        vm((wrows, 3 * width), F32),
        dma((2,)),
        vm((n_dom, 8, width), BF),
        vm((n_dom, 8, width), BF),
        vm((n_snap, block, width), BF),
        vm((n_snap, block, width), BF),
        vm((n_snap, block, width), BF),
        vm((n_snap, block, width), BF),
        vm((n_dom, 8, width), BF),
        vm((n_dom, 8, width), BF),
        vm((ny, 2, wrows, rows), BF),
        vm((ny, wrows, rows), BF),
        vm((rows, 3 * width), BF),
        vm((rows, 3 * width), BF),
        vm((nx, width // 2, cols), BF),
        vm((2, width // 2, cols), BF),
        vm((4, width // 4, cols), BF),
        vm((ny, wrows, cols), BF),
        vm((ny, wrows, cols), BF),
        vm((nz, xrows, 128), BF),
        vm((nz, xrows, 128), BF),
        vm((n_dom, xrows, 128), BF),
        vm((nz, ny, zrows, zcols), BF),
        vm((nz, ny, zrows, zcols), BF),
        vm((ny, zrows, zcols), BF),
        vm((ny, zrows, zcols), BF),
        vm((nx, zrows, zcols), BF),
        vm((nz, zrows, zcols), BF),
        vm((pairs, 2 * rows, 128), BF),
        vm((table, width), BF),
        vm((table, width), BF),
        vm((width, width), BF),
        vm((width, table), BF),
        vm((width, table), BF),
        vm((pairs, table, 2 * rows), F32),
        vm((pairs, table, 2 * rows), F32),
        vm((pairs, table, 2 * rows), BF),
        vm((pairs, table, 2 * rows), F32),
        vm((pairs, table, 2 * rows), BF),
        vm((pairs, 2 * rows, 128), BF),
        vm((width, rows), F32),
        vm((rows, width), F32),
        vm((table, 2 * width), BF),
        vm((rows, 2 * rows), F32),
        vm((rows, width), F32),
        vm((pairs, 2 * rows, 128), BF),
        vm((rows, 3 * width), BF),
        vm((pairs, 2 * rows, 128), BF),
        vm((pairs, rows, 2 * rows), F32),
        vm((pairs, rows, 2 * rows), F32),
        vm((pairs, rows, 2 * rows), BF),
        vm((pairs, rows, 2 * rows), BF),
        dma((2, n_dom)),
        dma((2, n_snap)),
        dma((2, n_snap)),
        dma((2, n_dom)),
        dma((2, 2)),
        dma((2, 6)),
        dma((2, ny)),
        dma((2, nz)),
        dma((2, n_dom)),
        dma((2, nz)),
        dma((2, ny)),
        dma((2, nx)),
        dma((2, nz)),
    ]
    in_vmem = pl.BlockSpec(memory_space=pltpu.VMEM)
    in_any = pl.BlockSpec(memory_space=pl.ANY)
    grad, gw = pl.pallas_call(
        functools.partial(kernel, (nz, nx, ny)),
        out_shape=(
            jax.ShapeDtypeStruct((rows, width), BF),
            jax.ShapeDtypeStruct((wrows, 3 * width), F32),
        ),
        in_specs=[in_any] * len(arrays),
        out_specs=(in_any,) * 2,
        scratch_shapes=scratch,
        compiler_params=pltpu.CompilerParams(collective_id=0, has_side_effects=True),
        name="step",
    )(*arrays)
    grad, gw = pl.pallas_call(
        emit,
        out_shape=(
            jax.ShapeDtypeStruct(grad.shape, BF),
            jax.ShapeDtypeStruct(gw.shape, F32),
        ),
        in_specs=[in_vmem] * 2,
        out_specs=(in_vmem,) * 2,
        name="emit",
    )(grad, gw)
    return (grad[None], gw)


def solution(mesh):
    return jax.shard_map(
        per_device,
        mesh=mesh,
        in_specs=(
            P("snap", "dom", None),
            P(),
            P(),
            P(),
            P(),
            P("snap", "dom", None),
            P("snap", "dom", None),
            P("snap", "dom", None, None),
            P(None, ("dom", "snap")),
            P(None, ("dom", "snap"), None),
        ),
        out_specs=(P("snap", "dom", None), P("snap", None)),
        check_vma=False,
    )
```

```python
import functools

import jax
import jax.numpy as jnp
from jax import lax
from jax.experimental import pallas as pl
from jax.experimental.pallas import tpu as pltpu
from jax.sharding import PartitionSpec as P

HEADS = 8
MESH = pl.DeviceIdType.MESH
BF = jnp.bfloat16
F32 = jnp.float32
GRID = {32: (8, 4), 4: (2, 2), 8: (2, 4)}


def mm(a, b):
    return jnp.dot(a, b, preferred_element_type=F32)


def mm_nt(a, b):
    return lax.dot_general(a, b, (((1,), (1,)), ((), ())), preferred_element_type=F32)


def mm_tn(a, b):
    return lax.dot_general(a, b, (((0,), (0,)), ((), ())), preferred_element_type=F32)


def iota(shape, axis):
    return lax.broadcasted_iota(jnp.int32, shape, axis)


def where_bf(mask, value):
    return jnp.where(mask, value, jnp.zeros_like(value))


def copy_to(src, dst, send_sem, recv_sem, device):
    return pltpu.make_async_remote_copy(
        src_ref=src,
        dst_ref=dst,
        send_sem=send_sem,
        recv_sem=recv_sem,
        device_id=device,
        device_id_type=MESH,
    )


def ring(shift, size):
    return min(shift, size - shift)


def far_first(dims):
    shifts = [()]
    for size in dims:
        shifts = [s + (i,) for s in shifts for i in range(abs(size))]
    hops = lambda s: sum(ring(i, n) if n > 0 else 0.1 * i for i, n in zip(s, dims))
    return sorted((s for s in shifts if any(s)), key=lambda s: -hops(s))


def moved(me, shift, dims):
    index = 0
    for at, step, size in zip(me, shift, dims):
        index = index * abs(size) + (lax.rem(at + step, abs(size)) if step else at)
    return index


class Exchange:
    def __init__(self, dims, me, device_of, src, dst, sems):
        self.dims, self.at, self.device_of = dims, me, device_of
        self.shifts = far_first(dims)
        self.me = moved(me, (0,) * len(dims), dims)
        self.count = len(self.shifts) + 1
        self.src, self.dst, self.send, self.recv = src, dst, sems.at[0], sems.at[1]

    def start(self):
        for shift in self.shifts:
            peer = moved(self.at, shift, self.dims)
            copy_to(
                self.src(peer),
                self.dst.at[self.me],
                self.send,
                self.recv,
                self.device_of(peer),
            ).start()

    def all_copies(self):
        others = self.dst.at[pl.ds(0, self.count - 1)]
        peer = moved(self.at, self.shifts[-1], self.dims)
        return copy_to(others, others, self.send, self.recv, self.device_of(peer))

    def wait_recv(self):
        if self.count > 1:
            self.all_copies().wait_recv()

    def wait_send(self):
        if self.count > 1:
            self.all_copies().wait_send()


def kernel(
    sizes,
    x_hbm,
    ws_hbm,
    wt_hbm,
    pos_hbm,
    rb_hbm,
    nbr_hbm,
    rel_hbm,
    send_hbm,
    act_hbm,
    ct_hbm,
    out_hbm,
    gw_hbm,
    x_ref,
    ws_ref,
    wt_ref,
    pos_ref,
    rb_ref,
    nbr_ref,
    rel_ref,
    send_ref,
    act_ref,
    ct_ref,
    in_sem,
    out_ref,
    gw_ref,
    out_sem,
    halo_s,
    halo_r,
    hid_s,
    hid_r,
    dh_s,
    dh_r,
    back_s,
    back_r,
    zt,
    zt_p,
    dt,
    dt_p,
    gx_s,
    gx_r,
    xy_s,
    xy_r,
    xz_r,
    xa_r,
    zz_s,
    zz_r,
    zy_s,
    zy_r,
    zx_r,
    za_r,
    qst,
    ktab,
    vtab,
    wvt,
    vt,
    ktt,
    cmat,
    attn,
    attn_b,
    d_att,
    d_sc,
    das,
    agg_t,
    slope,
    dkv,
    allow,
    pos_rows,
    cts,
    tp,
    tqs,
    t_s,
    t_d,
    t_w,
    t_b,
    halo_sem,
    hid_sem,
    dh_sem,
    back_sem,
    pair_sem,
    gx_sem,
    xy_sem,
    xz_sem,
    xa_sem,
    zz_sem,
    zy_sem,
    zx_sem,
    za_sem,
):
    nz, nx, ny = sizes
    n_dom, n_snap = nz * nx, 2 * ny
    rows, width = x_ref.shape
    halo = n_dom * 8
    table = rows + halo
    block = rows // n_snap
    cols = 2 * width // nx
    wrows = width // n_snap
    zc = min(4, nz)
    zrows, zcols = wrows // (nz // zc), width // zc
    scale = (width // HEADS) ** -0.5
    scale_bf = jnp.asarray(scale, BF)
    pairs = HEADS // 2

    loads = {
        "send": (send_hbm, send_ref),
        "x": (x_hbm, x_ref),
        "ws": (ws_hbm, ws_ref),
        "nbr": (nbr_hbm, nbr_ref),
        "rel": (rel_hbm, rel_ref),
        "rb": (rb_hbm, rb_ref),
        "act": (act_hbm, act_ref),
        "pos": (pos_hbm, pos_ref),
        "ct": (ct_hbm, ct_ref),
        "wt": (wt_hbm, wt_ref),
    }
    order = list(loads)

    def input_copy(name):
        return pltpu.make_async_copy(*loads[name], in_sem.at[order.index(name)])

    def arrive(name, load=True):
        input_copy(name).wait()
        return loads[name][1][...] if load else None

    for name in order:
        input_copy(name).start()

    me_d = lax.axis_index("dom")
    me_s = lax.axis_index("snap")
    me_z, me_x = me_d // nx, lax.rem(me_d, nx)
    me_y, me_c = me_s // 2, lax.rem(me_s, 2)
    partner = {"snap": me_s + 1 - 2 * me_c}

    barrier = pltpu.get_barrier_semaphore()

    for step in range(1, n_dom):
        pl.semaphore_signal(
            barrier, inc=1, device_id={"dom": lax.rem(me_d + step, n_dom)}, device_id_type=MESH
        )
    for step in range(1, n_snap):
        pl.semaphore_signal(
            barrier, inc=1, device_id={"snap": lax.rem(me_s + step, n_snap)}, device_id_type=MESH
        )

    dom, dom_at = (nz, nx), (me_z, me_x)
    snap, snap_at = (ny, -2), (me_y, me_c)
    to_dom = lambda p: {"dom": p}
    to_snap = lambda p: {"snap": p}
    to_x = lambda p: {"dom": me_z * nx + p}
    to_z = lambda p: {"dom": p * nx + me_x}
    to_y = lambda p: {"snap": p * 2 + me_c}
    halo_x = Exchange(dom, dom_at, to_dom, lambda p: halo_s.at[p], halo_r, halo_sem)
    hid_x = Exchange(snap, snap_at, to_snap, lambda p: hid_s.at[p], hid_r, hid_sem)
    dh_x = Exchange(snap, snap_at, to_snap, lambda p: dh_s.at[p], dh_r, dh_sem)
    back_x = Exchange(dom, dom_at, to_dom, lambda p: back_s.at[p], back_r, back_sem)
    px_x = Exchange((nx,), (me_x,), to_x, lambda p: gx_s.at[p], gx_r, gx_sem)
    py_x = Exchange((ny,), (me_y,), to_y, lambda p: xy_s.at[p], xy_r, xy_sem)
    pz_x = Exchange((nz,), (me_z,), to_z, lambda p: xz_r.at[me_z], xz_r, xz_sem)
    pa_x = Exchange((nx,), (me_x,), to_x, lambda p: xa_r.at[me_x], xa_r, xa_sem)
    qz_x = Exchange((nz,), (me_z,), to_z, lambda p: zz_s.at[p], zz_r, zz_sem)
    qy_x = Exchange((ny,), (me_y,), to_y, lambda p: zy_s.at[p], zy_r, zy_sem)
    qx_x = Exchange((nx,), (me_x,), to_x, lambda p: zx_r.at[me_x], zx_r, zx_sem)
    qa_x = Exchange((nz,), (me_z,), to_z, lambda p: za_r.at[me_z], za_r, za_sem)
    pair = [
        copy_to(zt.at[:, 1 - me_c], zt_p, pair_sem.at[0, 3], pair_sem.at[1, 3], partner)
    ] + [
        copy_to(dt.at[i], dt_p.at[i], pair_sem.at[0, i], pair_sem.at[1, i], partner)
        for i in range(3)
    ]

    send_f = arrive("send").astype(F32).astype(BF)
    spread = (iota((n_dom, halo), 1) // 8 == iota((n_dom, halo), 0)).astype(F32).astype(BF)
    wide = mm(send_f, spread)
    picked = jnp.where(lax.rem(iota((8, halo), 1), 8) == iota((8, halo), 0), wide, 0.0)
    send_row = jnp.sum(picked, axis=0, keepdims=True)
    pick_t = (iota((rows, halo), 0).astype(F32) == send_row).astype(F32)
    pick = pick_t.T.astype(BF)
    x_val = arrive("x")
    tiles = mm(pick, x_val)
    halo_s[...] = tiles.reshape(n_dom, 8, width).astype(BF)

    pl.semaphore_wait(barrier, n_dom + n_snap - 2)
    halo_x.start()
    halo_r[me_d] = halo_s[me_d]

    half = iota((rows, 128), 1) < 64

    def stack(value):
        zero = jnp.zeros_like(value)
        return jnp.concatenate(
            [jnp.where(half, value, zero), jnp.where(half, zero, value)], axis=0
        )

    w_v = pl.ds(2 * width, width)
    arrive("ws", load=False)
    own = mm(x_val, ws_ref[...]).astype(BF)
    ktab[0:rows, :] = own[:, width : 2 * width]
    vtab[0:rows, :] = own[:, 2 * width :]
    for p in range(pairs):
        qst[p] = stack(own[:, 128 * p : 128 * p + 128] * scale_bf)
    wvt[...] = ws_ref[:, w_v].T
    vt[:, 0:rows] = mm_nt(wvt[...], x_val).astype(BF)

    nbr = arrive("nbr").astype(F32)
    slots = nbr.shape[0]
    place = (1 << (4 * arrive("rel"))).astype(F32)
    row_t = iota((table, rows), 0).astype(F32)
    packed = jnp.zeros((table, rows), F32)
    for k in range(slots):
        packed += jnp.where(row_t == nbr[k : k + 1, :], place[k : k + 1, :], 0.0)
    packed = packed.astype(jnp.int32)
    counts = [((packed >> (4 * r)) & 15).astype(F32) for r in range(4)]
    eb = jnp.exp(arrive("rb"))
    for h in range(HEADS):
        total = counts[0] * eb[0:1, h : h + 1]
        for r in range(1, 4):
            total += counts[r] * eb[r : r + 1, h : h + 1]
        cmat[h // 2, :, (h % 2) * rows : (h % 2) * rows + rows] = total

    row_i = iota((rows, rows), 0)
    col_i = iota((rows, rows), 1)
    act_f = arrive("act").astype(F32).astype(BF)
    over = (iota((n_snap, rows), 1) // block == iota((n_snap, rows), 0)).astype(F32)
    act_w = mm(act_f, over.astype(BF))
    act_own = lax.rem(iota((block, rows), 1), block) == iota((block, rows), 0)
    act_row = jnp.sum(jnp.where(act_own, act_w, 0.0), axis=0, keepdims=True)
    same = lax.rem(row_i, block) == lax.rem(col_i, block)
    earlier = jnp.where(col_i // block <= row_i // block, act_row, 0.0)
    allowed = jnp.where(row_i == col_i, 1.0, jnp.where(same, earlier, 0.0)).T
    allow[:, 0:rows] = allowed
    allow[:, rows:] = allowed
    step_1h = (iota((rows, n_snap), 0) // block == iota((rows, n_snap), 1)).astype(F32)
    pos_rows[...] = mm(step_1h.astype(BF), arrive("pos"))
    ct_f = arrive("ct").astype(F32).reshape(rows, width)
    ct = ct_f.astype(BF)
    for p in range(pairs):
        cts[p] = stack(ct[:, 128 * p : 128 * p + 128])

    halo_x.wait_recv()
    halo_rows = halo_r[...].astype(F32).reshape(halo, width).astype(BF)
    ktab[rows:, :] = mm(halo_rows, ws_ref[:, width : 2 * width]).astype(BF)
    vt[:, rows:] = mm_nt(wvt[...], halo_rows).astype(BF)

    for p in range(pairs):
        attn[p] = mm_nt(ktab[:, 128 * p : 128 * p + 128], qst[p])
    for p in range(pairs):
        c = cmat[p]
        score = jnp.where(c > 0, attn[p], -1e30)
        e = jnp.exp(score - jnp.max(score, axis=0, keepdims=True)) * c
        w = e * (1.0 / jnp.sum(e, axis=0, keepdims=True))
        attn[p] = w
        attn_b[p] = w.astype(BF)
    for p in range(pairs):
        o = mm(vt[128 * p : 128 * p + 128, :], attn_b[p])
        agg_t[128 * p : 128 * p + 64, :] = o[0:64, 0:rows]
        agg_t[128 * p + 64 : 128 * p + 128, :] = o[64:128, rows:]
    agg = agg_t[...].T
    hidden = x_val.astype(F32) + jnp.where(agg > 0, agg, jnp.exp(jnp.minimum(agg, 0.0)) - 1.0)
    hid_s[...] = hidden.reshape(n_snap, block, width).astype(BF)
    hid_x.start()
    hid_r[me_s] = hid_s[me_s]
    slope[...] = jnp.where(agg > 0, 1.0, jnp.exp(jnp.minimum(agg, 0.0)))
    vtab[rows:, :] = mm(halo_rows, ws_ref[:, w_v]).astype(BF)
    ktt[...] = ktab[...].T
    arrive("wt", load=False)
    halo_x.wait_send()

    hid_x.wait_recv()
    z_f = hid_r[...].astype(F32).reshape(rows, width) + pos_rows[...]
    z = z_f.astype(BF)
    tp[...] = mm(z, wt_ref[...]).astype(BF)
    zt[...] = z_f.T.astype(BF).reshape(ny, 2, width // n_snap, rows)
    pair[0].start()
    for p in range(pairs):
        tqs[p] = stack(tp[:, 128 * p : 128 * p + 128] * scale_bf)
        t_s[p] = mm_nt(tp[:, width + 128 * p : width + 128 * p + 128], tqs[p])
        t_d[p] = mm_nt(tp[:, 2 * width + 128 * p : 2 * width + 128 * p + 128], cts[p])
    for p in range(pairs):
        score = jnp.where(allow[...] > 0, t_s[p], -1e30)
        e = jnp.exp(score - jnp.max(score, axis=0, keepdims=True))
        w = e * (1.0 / jnp.sum(e, axis=0, keepdims=True))
        t = w * t_d[p]
        t_w[p] = w.astype(BF)
        t_b[p] = (t - w * jnp.sum(t, axis=0, keepdims=True)).astype(BF)
    for p in range(pairs):
        dt[2, :, 128 * p : 128 * p + 128] = mm(t_w[p], cts[p]).astype(BF)
    pair[3].start()
    for p in range(pairs):
        dt[1, :, 128 * p : 128 * p + 128] = mm(t_b[p], tqs[p]).astype(BF)
    pair[2].start()
    for p in range(pairs):
        at = 128 * p
        dq = mm_tn(t_b[p], tp[:, width + at : width + at + 128]) * scale
        dt[0, :, at : at + 128] = jnp.where(half, dq[0:rows], dq[rows:]).astype(BF)
    pair[1].start()

    d_z = ct_f
    for i in range(3):
        d_z += mm_nt(dt[i], wt_ref[:, width * i : width * i + width])
    dh_s[...] = d_z.reshape(n_snap, block, width).astype(BF)
    dh_x.start()
    dh_r[me_s] = dh_s[me_s]

    pair[0].wait_recv()
    z_both = jnp.concatenate(
        [zt[:, me_c].reshape(width // 2, rows), zt_p[...].reshape(width // 2, rows)], axis=1
    )
    pair[3].wait_recv()
    product = mm(z_both, jnp.concatenate([dt[2], dt_p[2]], axis=0)).reshape(ny, wrows, width)
    for i in range(nz):
        r, c = i // zc * zrows, i % zc * zcols
        zz_s[i] = product[:, r : r + zrows, c : c + zcols].astype(BF)
    qz_x.start()
    zz_r[me_z] = zz_s[me_z]
    pair[2].wait_recv()
    pair[1].wait_recv()
    for i in range(nx):
        part, c = i * cols // width, i * cols % width
        d_both = jnp.concatenate([dt[part, :, c : c + cols], dt_p[part, :, c : c + cols]], axis=0)
        gx_s[i] = mm(z_both, d_both).astype(BF)
    px_x.start()

    hid_x.wait_send()
    dh_x.wait_recv()
    dh_f = dh_r[...].astype(F32).reshape(rows, width)
    d_agg = (dh_f * slope[...]).astype(BF)
    for p in range(pairs):
        das[p] = stack(d_agg[:, 128 * p : 128 * p + 128])
        d_att[p] = mm_nt(vtab[:, 128 * p : 128 * p + 128], das[p])
    for p in range(pairs):
        w = attn[p]
        t = w * d_att[p]
        d_sc[p] = (t - w * jnp.sum(t, axis=0, keepdims=True)).astype(BF)
    for p in range(pairs):
        at = 128 * p
        dkv[rows:, at : at + 128] = mm(d_sc[p, rows:, :], qst[p]).astype(BF)
        dkv[rows:, width + at : width + at + 128] = mm(attn_b[p, rows:, :], das[p]).astype(BF)

    d_halo = mm_nt(dkv[rows:, :], ws_ref[:, width:])
    back_s[...] = d_halo.reshape(n_dom, 8, width).astype(BF)
    back_x.start()
    back_r[me_d] = back_s[me_d]

    px_x.wait_recv()
    total = gx_s[me_x].astype(F32)
    for i in range(1, nx):
        total += gx_r[lax.rem(me_x + i, nx)].astype(F32)
    xy_s[...] = total.astype(BF).reshape(ny, wrows, cols)
    py_x.start()
    xy_r[me_y] = xy_s[me_y]

    for p in range(pairs):
        at = 128 * p
        dkv[0:rows, at : at + 128] = mm(d_sc[p, 0:rows, :], qst[p]).astype(BF)
        dkv[0:rows, width + at : width + at + 128] = mm(attn_b[p, 0:rows, :], das[p]).astype(BF)
        o = mm(ktt[at : at + 128, :], d_sc[p]) * scale
        agg_t[at : at + 64, :] = o[0:64, 0:rows]
        agg_t[at + 64 : at + 128, :] = o[64:128, rows:]
    dq = agg_t[...].T.astype(BF)
    d_own = dh_f + mm_nt(dq, ws_ref[:, :width]) + mm_nt(dkv[0:rows, :], ws_ref[:, width:])
    dh_x.wait_send()
    px_x.wait_send()
    for copy in pair:
        copy.wait_send()

    def total_of(ref, count):
        total = ref[0].astype(F32)
        for i in range(1, count):
            total += ref[i].astype(F32)
        return total

    qz_x.wait_recv()
    zy_s[...] = total_of(zz_r, nz).astype(BF)
    qy_x.start()
    zy_r[me_y] = zy_s[me_y]

    py_x.wait_recv()
    xz_r[me_z] = total_of(xy_r, ny).astype(BF)
    pz_x.start()
    qz_x.wait_send()
    py_x.wait_send()

    qy_x.wait_recv()
    zx_r[me_x] = total_of(zy_r, ny).astype(BF)
    qx_x.start()
    qy_x.wait_send()

    back_x.wait_recv()
    came = back_r[...].astype(F32).reshape(halo, width).astype(BF)
    out_ref[...] = (d_own + mm(pick_t.astype(BF), came)).astype(BF)
    save_out = pltpu.make_async_copy(out_ref, out_hbm, out_sem.at[0])
    save_out.start()

    pz_x.wait_recv()
    xa_r[me_x] = total_of(xz_r, nz).astype(BF)
    pa_x.start()
    qx_x.wait_recv()
    za_r[me_z] = total_of(zx_r, nx).astype(BF)
    qa_x.start()
    back_x.wait_send()
    pz_x.wait_send()
    qx_x.wait_send()
    qa_x.wait_recv()
    for i in range(nz):
        r, c = i // zc * zrows, 2 * width + i % zc * zcols
        gw_ref[r : r + zrows, c : c + zcols] = za_r[i].astype(F32)
    pa_x.wait_recv()
    for i in range(nx):
        gw_ref[:, cols * i : cols * i + cols] = xa_r[i].astype(F32)
    save_gw = pltpu.make_async_copy(gw_ref, gw_hbm, out_sem.at[1])
    save_gw.start()
    pa_x.wait_send()
    qa_x.wait_send()
    save_out.wait()
    save_gw.wait()


def emit(grad_in, gw_in, grad_out, gw_out, grad_v, gw_v, sem):
    first = pltpu.make_async_copy(gw_in, gw_v, sem.at[0])
    second = pltpu.make_async_copy(grad_in, grad_v, sem.at[1])
    first.start()
    second.start()
    first.wait()
    third = pltpu.make_async_copy(gw_v, gw_out, sem.at[2])
    third.start()
    second.wait()
    fourth = pltpu.make_async_copy(grad_v, grad_out, sem.at[3])
    fourth.start()
    third.wait()
    fourth.wait()


def per_device(
    feat, w_struct, w_temp, pos_embed, rel_bias, nbr, rel_type, send_idx, active, cotangent
):
    x = feat[0]
    rows, width = x.shape
    n_dom, n_snap = lax.axis_size("dom"), lax.axis_size("snap")
    nz, nx = GRID[n_dom]
    ny = n_snap // 2
    halo = n_dom * 8
    table = rows + halo
    block = rows // n_snap
    cols = 2 * width // nx
    wrows = width // n_snap
    zc = min(4, nz)
    zrows, zcols = wrows // (nz // zc), width // zc
    vm = pltpu.VMEM
    dma = pltpu.SemaphoreType.DMA
    arrays = (
        x,
        w_struct,
        w_temp,
        pos_embed,
        rel_bias,
        nbr[0].T,
        rel_type[0].T,
        send_idx[0, 0].T,
        active.T,
        cotangent,
    )
    pairs = HEADS // 2
    scratch = [vm(a.shape, a.dtype) for a in arrays] + [
        dma((len(arrays),)),
        vm((rows, width), BF),
        vm((wrows, 3 * width), F32),
        dma((2,)),
        vm((n_dom, 8, width), BF),
        vm((n_dom, 8, width), BF),
        vm((n_snap, block, width), BF),
        vm((n_snap, block, width), BF),
        vm((n_snap, block, width), BF),
        vm((n_snap, block, width), BF),
        vm((n_dom, 8, width), BF),
        vm((n_dom, 8, width), BF),
        vm((ny, 2, wrows, rows), BF),
        vm((ny, wrows, rows), BF),
        vm((3, rows, width), BF),
        vm((3, rows, width), BF),
        vm((nx, width // 2, cols), BF),
        vm((nx, width // 2, cols), BF),
        vm((ny, wrows, cols), BF),
        vm((ny, wrows, cols), BF),
        vm((nz, wrows, cols), BF),
        vm((nx, wrows, cols), BF),
        vm((nz, ny, zrows, zcols), BF),
        vm((nz, ny, zrows, zcols), BF),
        vm((ny, zrows, zcols), BF),
        vm((ny, zrows, zcols), BF),
        vm((nx, zrows, zcols), BF),
        vm((nz, zrows, zcols), BF),
        vm((pairs, 2 * rows, 128), BF),
        vm((table, width), BF),
        vm((table, width), BF),
        vm((width, width), BF),
        vm((width, table), BF),
        vm((width, table), BF),
        vm((pairs, table, 2 * rows), F32),
        vm((pairs, table, 2 * rows), F32),
        vm((pairs, table, 2 * rows), BF),
        vm((pairs, table, 2 * rows), F32),
        vm((pairs, table, 2 * rows), BF),
        vm((pairs, 2 * rows, 128), BF),
        vm((width, rows), F32),
        vm((rows, width), F32),
        vm((table, 2 * width), BF),
        vm((rows, 2 * rows), F32),
        vm((rows, width), F32),
        vm((pairs, 2 * rows, 128), BF),
        vm((rows, 3 * width), BF),
        vm((pairs, 2 * rows, 128), BF),
        vm((pairs, rows, 2 * rows), F32),
        vm((pairs, rows, 2 * rows), F32),
        vm((pairs, rows, 2 * rows), BF),
        vm((pairs, rows, 2 * rows), BF),
        dma((2,)),
        dma((2,)),
        dma((2,)),
        dma((2,)),
        dma((2, 4)),
        dma((2,)),
        dma((2,)),
        dma((2,)),
        dma((2,)),
        dma((2,)),
        dma((2,)),
        dma((2,)),
        dma((2,)),
    ]
    in_any = pl.BlockSpec(memory_space=pl.ANY)
    grad, gw = pl.pallas_call(
        functools.partial(kernel, (nz, nx, ny)),
        out_shape=(
            jax.ShapeDtypeStruct((rows, width), BF),
            jax.ShapeDtypeStruct((wrows, 3 * width), F32),
        ),
        in_specs=[in_any] * len(arrays),
        out_specs=(in_any,) * 2,
        scratch_shapes=scratch,
        compiler_params=pltpu.CompilerParams(
            collective_id=0, has_side_effects=True
        ),
        name="step",
    )(*arrays)
    grad, gw = pl.pallas_call(
        emit,
        out_shape=(
            jax.ShapeDtypeStruct(grad.shape, BF),
            jax.ShapeDtypeStruct(gw.shape, F32),
        ),
        in_specs=[in_any] * 2,
        out_specs=(in_any,) * 2,
        scratch_shapes=[vm(grad.shape, BF), vm(gw.shape, F32), dma((4,))],
        name="emit",
    )(grad, gw)
    return (grad[None], gw)


def solution(mesh):
    return jax.shard_map(
        per_device,
        mesh=mesh,
        in_specs=(
            P("snap", "dom", None),
            P(),
            P(),
            P(),
            P(),
            P("snap", "dom", None),
            P("snap", "dom", None),
            P("snap", "dom", None, None),
            P(None, ("dom", "snap")),
            P(None, ("dom", "snap"), None),
        ),
        out_specs=(P("snap", "dom", None), P("snap", None)),
        check_vma=False,
    )
```

```python
import functools

import jax
import jax.numpy as jnp
from jax import lax
from jax.experimental import pallas as pl
from jax.experimental.pallas import tpu as pltpu
from jax.sharding import PartitionSpec as P

HEADS = 8
MESH = pl.DeviceIdType.MESH
BF = jnp.bfloat16
F32 = jnp.float32
GRID = {32: (8, 4), 4: (2, 2), 8: (2, 4)}


def mm(a, b):
    return jnp.dot(a, b, preferred_element_type=F32)


def mm_nt(a, b):
    return lax.dot_general(a, b, (((1,), (1,)), ((), ())), preferred_element_type=F32)


def mm_tn(a, b):
    return lax.dot_general(a, b, (((0,), (0,)), ((), ())), preferred_element_type=F32)


def iota(shape, axis):
    return lax.broadcasted_iota(jnp.int32, shape, axis)


def where_bf(mask, value):
    return jnp.where(mask, value, jnp.zeros_like(value))


def copy_to(src, dst, send_sem, recv_sem, device):
    return pltpu.make_async_remote_copy(
        src_ref=src,
        dst_ref=dst,
        send_sem=send_sem,
        recv_sem=recv_sem,
        device_id=device,
        device_id_type=MESH,
    )


def ring(shift, size):
    return min(shift, size - shift)


def far_first(dims):
    shifts = [()]
    for size in dims:
        shifts = [s + (i,) for s in shifts for i in range(abs(size))]
    hops = lambda s: sum(ring(i, n) if n > 0 else 0.1 * i for i, n in zip(s, dims))
    return sorted((s for s in shifts if any(s)), key=lambda s: -hops(s))


def moved(me, shift, dims):
    index = 0
    for at, step, size in zip(me, shift, dims):
        index = index * abs(size) + (lax.rem(at + step, abs(size)) if step else at)
    return index


class Exchange:
    def __init__(self, dims, me, device_of, src, dst, sems):
        self.dims, self.at, self.device_of = dims, me, device_of
        self.shifts = far_first(dims)
        self.me = moved(me, (0,) * len(dims), dims)
        self.count = len(self.shifts) + 1
        self.src, self.dst, self.send, self.recv = src, dst, sems.at[0], sems.at[1]

    def start(self):
        for shift in self.shifts:
            peer = moved(self.at, shift, self.dims)
            copy_to(
                self.src(peer),
                self.dst.at[self.me],
                self.send,
                self.recv,
                self.device_of(peer),
            ).start()

    def all_copies(self):
        others = self.dst.at[pl.ds(0, self.count - 1)]
        peer = moved(self.at, self.shifts[-1], self.dims)
        return copy_to(others, others, self.send, self.recv, self.device_of(peer))

    def wait_recv(self):
        if self.count > 1:
            self.all_copies().wait_recv()

    def wait_send(self):
        if self.count > 1:
            self.all_copies().wait_send()


def kernel(
    sizes,
    x_hbm,
    ws_hbm,
    wt_hbm,
    pos_hbm,
    rb_hbm,
    nbr_hbm,
    rel_hbm,
    send_hbm,
    act_hbm,
    ct_hbm,
    out_hbm,
    gw_hbm,
    x_ref,
    ws_ref,
    wt_ref,
    pos_ref,
    rb_ref,
    nbr_ref,
    rel_ref,
    send_ref,
    act_ref,
    ct_ref,
    in_sem,
    out_ref,
    gw_ref,
    out_sem,
    halo_s,
    halo_r,
    hid_s,
    hid_r,
    dh_s,
    dh_r,
    back_s,
    back_r,
    zt,
    zt_p,
    dt,
    dt_p,
    gx_s,
    gx_r,
    xy_s,
    xy_r,
    xz_r,
    xa_r,
    zz_s,
    zz_r,
    zy_s,
    zy_r,
    zx_r,
    za_r,
    qst,
    ktab,
    vtab,
    wvt,
    vt,
    ktt,
    cmat,
    attn,
    attn_b,
    d_att,
    d_sc,
    das,
    agg_t,
    slope,
    dkv,
    allow,
    pos_rows,
    cts,
    tp,
    tqs,
    t_s,
    t_d,
    t_w,
    t_b,
    halo_sem,
    hid_sem,
    dh_sem,
    back_sem,
    pair_sem,
    gx_sem,
    xy_sem,
    xz_sem,
    xa_sem,
    zz_sem,
    zy_sem,
    zx_sem,
    za_sem,
):
    nz, nx, ny = sizes
    n_dom, n_snap = nz * nx, 2 * ny
    rows, width = x_ref.shape
    halo = n_dom * 8
    table = rows + halo
    block = rows // n_snap
    cols = 2 * width // nx
    wrows = width // n_snap
    zc = min(4, nz)
    zrows, zcols = wrows // (nz // zc), width // zc
    scale = (width // HEADS) ** -0.5
    scale_bf = jnp.asarray(scale, BF)
    pairs = HEADS // 2

    loads = {
        "send": (send_hbm, send_ref),
        "x": (x_hbm, x_ref),
        "ws": (ws_hbm, ws_ref),
        "nbr": (nbr_hbm, nbr_ref),
        "rel": (rel_hbm, rel_ref),
        "rb": (rb_hbm, rb_ref),
        "act": (act_hbm, act_ref),
        "pos": (pos_hbm, pos_ref),
        "ct": (ct_hbm, ct_ref),
        "wt": (wt_hbm, wt_ref),
    }
    order = list(loads)

    def input_copy(name):
        return pltpu.make_async_copy(*loads[name], in_sem.at[order.index(name)])

    def arrive(name, load=True):
        input_copy(name).wait()
        return loads[name][1][...] if load else None

    for name in order:
        input_copy(name).start()

    me_d = lax.axis_index("dom")
    me_s = lax.axis_index("snap")
    me_z, me_x = me_d // nx, lax.rem(me_d, nx)
    me_y, me_c = me_s // 2, lax.rem(me_s, 2)
    partner = {"snap": me_s + 1 - 2 * me_c}

    barrier = pltpu.get_barrier_semaphore()

    dom, dom_at = (nz, nx), (me_z, me_x)
    snap, snap_at = (ny, -2), (me_y, me_c)
    to_dom = lambda p: {"dom": p}
    to_snap = lambda p: {"snap": p}
    to_x = lambda p: {"dom": me_z * nx + p}
    to_z = lambda p: {"dom": p * nx + me_x}
    to_y = lambda p: {"snap": p * 2 + me_c}
    for shift in far_first(dom):
        peer = to_dom(moved(dom_at, shift, dom))
        pl.semaphore_signal(barrier, inc=1, device_id=peer, device_id_type=MESH)
    for shift in far_first(snap):
        peer = to_snap(moved(snap_at, shift, snap))
        pl.semaphore_signal(barrier, inc=1, device_id=peer, device_id_type=MESH)

    halo_x = Exchange(dom, dom_at, to_dom, lambda p: halo_s.at[p], halo_r, halo_sem)
    hid_x = Exchange(snap, snap_at, to_snap, lambda p: hid_s.at[p], hid_r, hid_sem)
    dh_x = Exchange(snap, snap_at, to_snap, lambda p: dh_s.at[p], dh_r, dh_sem)
    back_x = Exchange(dom, dom_at, to_dom, lambda p: back_s.at[p], back_r, back_sem)
    px_x = Exchange((nx,), (me_x,), to_x, lambda p: gx_s.at[p], gx_r, gx_sem)
    py_x = Exchange((ny,), (me_y,), to_y, lambda p: xy_s.at[p], xy_r, xy_sem)
    pz_x = Exchange((nz,), (me_z,), to_z, lambda p: xz_r.at[me_z], xz_r, xz_sem)
    pa_x = Exchange((nx,), (me_x,), to_x, lambda p: xa_r.at[me_x], xa_r, xa_sem)
    qz_x = Exchange((nz,), (me_z,), to_z, lambda p: zz_s.at[p], zz_r, zz_sem)
    qy_x = Exchange((ny,), (me_y,), to_y, lambda p: zy_s.at[p], zy_r, zy_sem)
    qx_x = Exchange((nx,), (me_x,), to_x, lambda p: zx_r.at[me_x], zx_r, zx_sem)
    qa_x = Exchange((nz,), (me_z,), to_z, lambda p: za_r.at[me_z], za_r, za_sem)
    pair = [
        copy_to(zt.at[:, 1 - me_c], zt_p, pair_sem.at[0, 3], pair_sem.at[1, 3], partner)
    ] + [
        copy_to(dt.at[i], dt_p.at[i], pair_sem.at[0, i], pair_sem.at[1, i], partner)
        for i in range(3)
    ]

    send_f = arrive("send").astype(F32).astype(BF)
    spread = (iota((n_dom, halo), 1) // 8 == iota((n_dom, halo), 0)).astype(F32).astype(BF)
    wide = mm(send_f, spread)
    picked = jnp.where(lax.rem(iota((8, halo), 1), 8) == iota((8, halo), 0), wide, 0.0)
    send_row = jnp.sum(picked, axis=0, keepdims=True)
    pick_t = (iota((rows, halo), 0).astype(F32) == send_row).astype(F32)
    pick = pick_t.T.astype(BF)
    x_val = arrive("x")
    tiles = mm(pick, x_val)
    halo_s[...] = tiles.reshape(n_dom, 8, width).astype(BF)

    pl.semaphore_wait(barrier, n_dom + n_snap - 2)
    halo_x.start()
    halo_r[me_d] = halo_s[me_d]

    half = iota((rows, 128), 1) < 64

    def stack(value):
        zero = jnp.zeros_like(value)
        return jnp.concatenate(
            [jnp.where(half, value, zero), jnp.where(half, zero, value)], axis=0
        )

    w_v = pl.ds(2 * width, width)
    arrive("ws", load=False)
    own = mm(x_val, ws_ref[...]).astype(BF)
    ktab[0:rows, :] = own[:, width : 2 * width]
    vtab[0:rows, :] = own[:, 2 * width :]
    for p in range(pairs):
        qst[p] = stack(own[:, 128 * p : 128 * p + 128] * scale_bf)
    wvt[...] = ws_ref[:, w_v].T
    vt[:, 0:rows] = mm_nt(wvt[...], x_val).astype(BF)

    nbr = arrive("nbr").astype(F32)
    slots = nbr.shape[0]
    place = (1 << (4 * arrive("rel"))).astype(F32)
    row_t = iota((table, rows), 0).astype(F32)
    packed = jnp.zeros((table, rows), F32)
    for k in range(slots):
        packed += jnp.where(row_t == nbr[k : k + 1, :], place[k : k + 1, :], 0.0)
    packed = packed.astype(jnp.int32)
    counts = [((packed >> (4 * r)) & 15).astype(F32) for r in range(4)]
    eb = jnp.exp(arrive("rb"))
    for h in range(HEADS):
        total = counts[0] * eb[0:1, h : h + 1]
        for r in range(1, 4):
            total += counts[r] * eb[r : r + 1, h : h + 1]
        cmat[h // 2, :, (h % 2) * rows : (h % 2) * rows + rows] = jnp.where(
            packed > 0, jnp.log(total), -1e30
        )

    row_i = iota((rows, rows), 0)
    col_i = iota((rows, rows), 1)
    act_f = arrive("act").astype(F32).astype(BF)
    over = (iota((n_snap, rows), 1) // block == iota((n_snap, rows), 0)).astype(F32)
    act_w = mm(act_f, over.astype(BF))
    act_own = lax.rem(iota((block, rows), 1), block) == iota((block, rows), 0)
    act_row = jnp.sum(jnp.where(act_own, act_w, 0.0), axis=0, keepdims=True)
    same = lax.rem(row_i, block) == lax.rem(col_i, block)
    earlier = jnp.where(col_i // block <= row_i // block, act_row, 0.0)
    allowed = jnp.where(row_i == col_i, 1.0, jnp.where(same, earlier, 0.0)).T
    allow[:, 0:rows] = allowed
    allow[:, rows:] = allowed
    step_1h = (iota((rows, n_snap), 0) // block == iota((rows, n_snap), 1)).astype(F32)
    pos_rows[...] = mm(step_1h.astype(BF), arrive("pos"))
    ct_f = arrive("ct").astype(F32).reshape(rows, width)
    ct = ct_f.astype(BF)
    for p in range(pairs):
        cts[p] = stack(ct[:, 128 * p : 128 * p + 128])

    halo_x.wait_recv()
    halo_rows = halo_r[...].astype(F32).reshape(halo, width).astype(BF)
    ktab[rows:, :] = mm(halo_rows, ws_ref[:, width : 2 * width]).astype(BF)
    vt[:, rows:] = mm_nt(wvt[...], halo_rows).astype(BF)

    for p in range(pairs):
        attn[p] = mm_nt(ktab[:, 128 * p : 128 * p + 128], qst[p])
    for p in range(pairs):
        score = attn[p] + cmat[p]
        e = jnp.exp(score - jnp.max(score, axis=0, keepdims=True))
        w = e * (1.0 / jnp.sum(e, axis=0, keepdims=True))
        attn[p] = w
        attn_b[p] = w.astype(BF)
    for p in range(pairs):
        o = mm(vt[128 * p : 128 * p + 128, :], attn_b[p])
        agg_t[128 * p : 128 * p + 64, :] = o[0:64, 0:rows]
        agg_t[128 * p + 64 : 128 * p + 128, :] = o[64:128, rows:]
    agg = agg_t[...].T
    hidden = x_val.astype(F32) + jnp.where(agg > 0, agg, jnp.exp(jnp.minimum(agg, 0.0)) - 1.0)
    hid_s[...] = hidden.reshape(n_snap, block, width).astype(BF)
    hid_x.start()
    hid_r[me_s] = hid_s[me_s]
    slope[...] = jnp.where(agg > 0, 1.0, jnp.exp(jnp.minimum(agg, 0.0)))
    vtab[rows:, :] = mm(halo_rows, ws_ref[:, w_v]).astype(BF)
    ktt[...] = ktab[...].T
    arrive("wt", load=False)
    halo_x.wait_send()

    hid_x.wait_recv()
    z_f = hid_r[...].astype(F32).reshape(rows, width) + pos_rows[...]
    z = z_f.astype(BF)
    tp[...] = mm(z, wt_ref[...]).astype(BF)
    zt[...] = z_f.T.astype(BF).reshape(ny, 2, width // n_snap, rows)
    pair[0].start()
    for p in range(pairs):
        tqs[p] = stack(tp[:, 128 * p : 128 * p + 128] * scale_bf)
        t_s[p] = mm_nt(tp[:, width + 128 * p : width + 128 * p + 128], tqs[p])
        t_d[p] = mm_nt(tp[:, 2 * width + 128 * p : 2 * width + 128 * p + 128], cts[p])
    for p in range(pairs):
        score = jnp.where(allow[...] > 0, t_s[p], -1e30)
        e = jnp.exp(score - jnp.max(score, axis=0, keepdims=True))
        w = e * (1.0 / jnp.sum(e, axis=0, keepdims=True))
        t = w * t_d[p]
        t_w[p] = w.astype(BF)
        t_b[p] = (t - w * jnp.sum(t, axis=0, keepdims=True)).astype(BF)
    for p in range(pairs):
        dt[2, :, 128 * p : 128 * p + 128] = mm(t_w[p], cts[p]).astype(BF)
    pair[3].start()
    for p in range(pairs):
        dt[1, :, 128 * p : 128 * p + 128] = mm(t_b[p], tqs[p]).astype(BF)
    pair[2].start()
    for p in range(pairs):
        at = 128 * p
        dq = mm_tn(t_b[p], tp[:, width + at : width + at + 128]) * scale
        dt[0, :, at : at + 128] = jnp.where(half, dq[0:rows], dq[rows:]).astype(BF)
    pair[1].start()

    d_z = ct_f
    for i in range(3):
        d_z += mm_nt(dt[i], wt_ref[:, width * i : width * i + width])
    dh_s[...] = d_z.reshape(n_snap, block, width).astype(BF)
    dh_x.start()
    dh_r[me_s] = dh_s[me_s]

    pair[0].wait_recv()
    z_both = jnp.concatenate(
        [zt[:, me_c].reshape(width // 2, rows), zt_p[...].reshape(width // 2, rows)], axis=1
    )
    pair[3].wait_recv()
    product = mm(z_both, jnp.concatenate([dt[2], dt_p[2]], axis=0)).reshape(ny, wrows, width)
    for i in range(nz):
        r, c = i // zc * zrows, i % zc * zcols
        zz_s[i] = product[:, r : r + zrows, c : c + zcols].astype(BF)
    qz_x.start()
    zz_r[me_z] = zz_s[me_z]
    pair[2].wait_recv()
    pair[1].wait_recv()
    for i in range(nx):
        part, c = i * cols // width, i * cols % width
        d_both = jnp.concatenate([dt[part, :, c : c + cols], dt_p[part, :, c : c + cols]], axis=0)
        gx_s[i] = mm(z_both, d_both).astype(BF)
    px_x.start()

    hid_x.wait_send()
    dh_x.wait_recv()
    dh_f = dh_r[...].astype(F32).reshape(rows, width)
    d_agg = (dh_f * slope[...]).astype(BF)
    for p in range(pairs):
        das[p] = stack(d_agg[:, 128 * p : 128 * p + 128])
        d_att[p] = mm_nt(vtab[:, 128 * p : 128 * p + 128], das[p])
    for p in range(pairs):
        w = attn[p]
        t = w * d_att[p]
        d_sc[p] = (t - w * jnp.sum(t, axis=0, keepdims=True)).astype(BF)
    for p in range(pairs):
        at = 128 * p
        dkv[rows:, at : at + 128] = mm(d_sc[p, rows:, :], qst[p]).astype(BF)
        dkv[rows:, width + at : width + at + 128] = mm(attn_b[p, rows:, :], das[p]).astype(BF)

    d_halo = mm_nt(dkv[rows:, :], ws_ref[:, width:])
    back_s[...] = d_halo.reshape(n_dom, 8, width).astype(BF)
    back_x.start()
    back_r[me_d] = back_s[me_d]

    def total_of(ref, count):
        total = ref[0].astype(F32)
        for i in range(1, count):
            total += ref[i].astype(F32)
        return total

    qz_x.wait_recv()
    zy_s[...] = total_of(zz_r, nz).astype(BF)
    qy_x.start()
    zy_r[me_y] = zy_s[me_y]

    px_x.wait_recv()
    total = gx_s[me_x].astype(F32)
    for i in range(1, nx):
        total += gx_r[lax.rem(me_x + i, nx)].astype(F32)
    xy_s[...] = total.astype(BF).reshape(ny, wrows, cols)
    py_x.start()
    xy_r[me_y] = xy_s[me_y]

    for p in range(pairs):
        at = 128 * p
        dkv[0:rows, at : at + 128] = mm(d_sc[p, 0:rows, :], qst[p]).astype(BF)
        dkv[0:rows, width + at : width + at + 128] = mm(attn_b[p, 0:rows, :], das[p]).astype(BF)
        o = mm(ktt[at : at + 128, :], d_sc[p]) * scale
        agg_t[at : at + 64, :] = o[0:64, 0:rows]
        agg_t[at + 64 : at + 128, :] = o[64:128, rows:]
    dq = agg_t[...].T.astype(BF)
    d_own = dh_f + mm_nt(dq, ws_ref[:, :width]) + mm_nt(dkv[0:rows, :], ws_ref[:, width:])
    dh_x.wait_send()
    px_x.wait_send()
    for copy in pair:
        copy.wait_send()

    qy_x.wait_recv()
    zx_r[me_x] = total_of(zy_r, ny).astype(BF)
    qx_x.start()
    qy_x.wait_send()

    py_x.wait_recv()
    xz_r[me_z] = total_of(xy_r, ny).astype(BF)
    pz_x.start()
    qz_x.wait_send()
    py_x.wait_send()

    back_x.wait_recv()
    came = back_r[...].astype(F32).reshape(halo, width).astype(BF)
    out_ref[...] = (d_own + mm(pick_t.astype(BF), came)).astype(BF)
    save_out = pltpu.make_async_copy(out_ref, out_hbm, out_sem.at[0])
    save_out.start()

    qx_x.wait_recv()
    za_r[me_z] = total_of(zx_r, nx).astype(BF)
    qa_x.start()
    pz_x.wait_recv()
    xa_r[me_x] = total_of(xz_r, nz).astype(BF)
    pa_x.start()
    back_x.wait_send()
    pz_x.wait_send()
    qx_x.wait_send()
    qa_x.wait_recv()
    for i in range(nz):
        r, c = i // zc * zrows, 2 * width + i % zc * zcols
        gw_ref[r : r + zrows, c : c + zcols] = za_r[i].astype(F32)
    pa_x.wait_recv()
    for i in range(nx):
        gw_ref[:, cols * i : cols * i + cols] = xa_r[i].astype(F32)
    save_gw = pltpu.make_async_copy(gw_ref, gw_hbm, out_sem.at[1])
    save_gw.start()
    pa_x.wait_send()
    qa_x.wait_send()
    save_out.wait()
    save_gw.wait()


def emit(grad_in, gw_in, grad_out, gw_out, sem):
    first = pltpu.make_async_copy(gw_in, gw_out, sem.at[0])
    second = pltpu.make_async_copy(grad_in, grad_out, sem.at[1])
    first.start()
    second.start()
    first.wait()
    second.wait()


def per_device(
    feat, w_struct, w_temp, pos_embed, rel_bias, nbr, rel_type, send_idx, active, cotangent
):
    x = feat[0]
    rows, width = x.shape
    n_dom, n_snap = lax.axis_size("dom"), lax.axis_size("snap")
    nz, nx = GRID[n_dom]
    ny = n_snap // 2
    halo = n_dom * 8
    table = rows + halo
    block = rows // n_snap
    cols = 2 * width // nx
    wrows = width // n_snap
    zc = min(4, nz)
    zrows, zcols = wrows // (nz // zc), width // zc
    vm = pltpu.VMEM
    dma = pltpu.SemaphoreType.DMA
    arrays = (
        x,
        w_struct,
        w_temp,
        pos_embed,
        rel_bias,
        nbr[0].T,
        rel_type[0].T,
        send_idx[0, 0].T,
        active.T,
        cotangent,
    )
    pairs = HEADS // 2
    scratch = [vm(a.shape, a.dtype) for a in arrays] + [
        dma((len(arrays),)),
        vm((rows, width), BF),
        vm((wrows, 3 * width), F32),
        dma((2,)),
        vm((n_dom, 8, width), BF),
        vm((n_dom, 8, width), BF),
        vm((n_snap, block, width), BF),
        vm((n_snap, block, width), BF),
        vm((n_snap, block, width), BF),
        vm((n_snap, block, width), BF),
        vm((n_dom, 8, width), BF),
        vm((n_dom, 8, width), BF),
        vm((ny, 2, wrows, rows), BF),
        vm((ny, wrows, rows), BF),
        vm((3, rows, width), BF),
        vm((3, rows, width), BF),
        vm((nx, width // 2, cols), BF),
        vm((nx, width // 2, cols), BF),
        vm((ny, wrows, cols), BF),
        vm((ny, wrows, cols), BF),
        vm((nz, wrows, cols), BF),
        vm((nx, wrows, cols), BF),
        vm((nz, ny, zrows, zcols), BF),
        vm((nz, ny, zrows, zcols), BF),
        vm((ny, zrows, zcols), BF),
        vm((ny, zrows, zcols), BF),
        vm((nx, zrows, zcols), BF),
        vm((nz, zrows, zcols), BF),
        vm((pairs, 2 * rows, 128), BF),
        vm((table, width), BF),
        vm((table, width), BF),
        vm((width, width), BF),
        vm((width, table), BF),
        vm((width, table), BF),
        vm((pairs, table, 2 * rows), F32),
        vm((pairs, table, 2 * rows), F32),
        vm((pairs, table, 2 * rows), BF),
        vm((pairs, table, 2 * rows), F32),
        vm((pairs, table, 2 * rows), BF),
        vm((pairs, 2 * rows, 128), BF),
        vm((width, rows), F32),
        vm((rows, width), F32),
        vm((table, 2 * width), BF),
        vm((rows, 2 * rows), F32),
        vm((rows, width), F32),
        vm((pairs, 2 * rows, 128), BF),
        vm((rows, 3 * width), BF),
        vm((pairs, 2 * rows, 128), BF),
        vm((pairs, rows, 2 * rows), F32),
        vm((pairs, rows, 2 * rows), F32),
        vm((pairs, rows, 2 * rows), BF),
        vm((pairs, rows, 2 * rows), BF),
        dma((2,)),
        dma((2,)),
        dma((2,)),
        dma((2,)),
        dma((2, 4)),
        dma((2,)),
        dma((2,)),
        dma((2,)),
        dma((2,)),
        dma((2,)),
        dma((2,)),
        dma((2,)),
        dma((2,)),
    ]
    in_any = pl.BlockSpec(memory_space=pl.ANY)
    grad, gw = pl.pallas_call(
        functools.partial(kernel, (nz, nx, ny)),
        out_shape=(
            jax.ShapeDtypeStruct((rows, width), BF),
            jax.ShapeDtypeStruct((wrows, 3 * width), F32),
        ),
        in_specs=[in_any] * len(arrays),
        out_specs=(in_any,) * 2,
        scratch_shapes=scratch,
        compiler_params=pltpu.CompilerParams(
            collective_id=0, has_side_effects=True, vmem_limit_bytes=48 * 2**20
        ),
        name="step",
    )(*[pltpu.with_memory_space_constraint(a, pltpu.HBM) for a in arrays])
    grad, gw = pl.pallas_call(
        emit,
        out_shape=(
            jax.ShapeDtypeStruct(grad.shape, BF),
            jax.ShapeDtypeStruct(gw.shape, F32),
        ),
        in_specs=[in_any] * 2,
        out_specs=(in_any,) * 2,
        scratch_shapes=[dma((2,))],
        compiler_params=pltpu.CompilerParams(vmem_limit_bytes=4 * 2**20),
        name="emit",
    )(grad, gw)
    return (grad[None], gw)


def solution(mesh):
    return jax.shard_map(
        per_device,
        mesh=mesh,
        in_specs=(
            P("snap", "dom", None),
            P(),
            P(),
            P(),
            P(),
            P("snap", "dom", None),
            P("snap", "dom", None),
            P("snap", "dom", None, None),
            P(None, ("dom", "snap")),
            P(None, ("dom", "snap"), None),
        ),
        out_specs=(P("snap", "dom", None), P("snap", None)),
        check_vma=False,
    )
```

```python
import functools

import jax
import jax.numpy as jnp
from jax import lax
from jax.experimental import pallas as pl
from jax.experimental.pallas import tpu as pltpu
from jax.sharding import PartitionSpec as P

HEADS = 8
MESH = pl.DeviceIdType.MESH
BF = jnp.bfloat16
F32 = jnp.float32
GRID = {32: (8, 4), 4: (2, 2), 8: (2, 4)}


def mm(a, b):
    return jnp.dot(a, b, preferred_element_type=F32)


def mm_nt(a, b):
    return lax.dot_general(a, b, (((1,), (1,)), ((), ())), preferred_element_type=F32)


def mm_tn(a, b):
    return lax.dot_general(a, b, (((0,), (0,)), ((), ())), preferred_element_type=F32)


def iota(shape, axis):
    return lax.broadcasted_iota(jnp.int32, shape, axis)


def where_bf(mask, value):
    return jnp.where(mask, value, jnp.zeros_like(value))


def copy_to(src, dst, send_sem, recv_sem, device):
    return pltpu.make_async_remote_copy(
        src_ref=src,
        dst_ref=dst,
        send_sem=send_sem,
        recv_sem=recv_sem,
        device_id=device,
        device_id_type=MESH,
    )


def ring(shift, size):
    return min(shift, size - shift)


def far_first(dims):
    shifts = [()]
    for size in dims:
        shifts = [s + (i,) for s in shifts for i in range(abs(size))]
    hops = lambda s: sum(ring(i, n) if n > 0 else 0.1 * i for i, n in zip(s, dims))
    return sorted((s for s in shifts if any(s)), key=lambda s: -hops(s))


def moved(me, shift, dims):
    index = 0
    for at, step, size in zip(me, shift, dims):
        index = index * abs(size) + (lax.rem(at + step, abs(size)) if step else at)
    return index


class Exchange:
    def __init__(self, dims, me, device_of, src, dst, sems):
        self.dims, self.at, self.device_of = dims, me, device_of
        self.shifts = far_first(dims)
        self.me = moved(me, (0,) * len(dims), dims)
        self.count = len(self.shifts) + 1
        self.src, self.dst, self.send, self.recv = src, dst, sems.at[0], sems.at[1]

    def start(self):
        for shift in self.shifts:
            peer = moved(self.at, shift, self.dims)
            copy_to(
                self.src(peer),
                self.dst.at[self.me],
                self.send,
                self.recv,
                self.device_of(peer),
            ).start()

    def all_copies(self):
        others = self.dst.at[pl.ds(0, self.count - 1)]
        peer = moved(self.at, self.shifts[-1], self.dims)
        return copy_to(others, others, self.send, self.recv, self.device_of(peer))

    def wait_recv(self):
        if self.count > 1:
            self.all_copies().wait_recv()

    def wait_send(self):
        if self.count > 1:
            self.all_copies().wait_send()


def kernel(
    sizes,
    x_hbm,
    ws_hbm,
    wt_hbm,
    pos_hbm,
    rb_hbm,
    nbr_hbm,
    rel_hbm,
    send_hbm,
    act_hbm,
    ct_hbm,
    out_hbm,
    gw_hbm,
    x_ref,
    ws_ref,
    wt_ref,
    pos_ref,
    rb_ref,
    nbr_ref,
    rel_ref,
    send_ref,
    act_ref,
    ct_ref,
    in_sem,
    out_ref,
    gw_ref,
    out_sem,
    halo_s,
    halo_r,
    hid_s,
    hid_r,
    dh_s,
    dh_r,
    back_s,
    back_r,
    zt,
    zt_p,
    dt,
    dt_p,
    gx_s,
    gx_r,
    xy_s,
    xy_r,
    xz_r,
    xa_r,
    zz_s,
    zz_r,
    zy_s,
    zy_r,
    zx_r,
    za_r,
    qst,
    ktab,
    vtab,
    wvt,
    vt,
    ktt,
    cmat,
    attn,
    attn_b,
    d_att,
    d_sc,
    das,
    agg_t,
    slope,
    dkv,
    allow,
    pos_rows,
    cts,
    tp,
    tqs,
    t_s,
    t_d,
    t_w,
    t_b,
    halo_sem,
    hid_sem,
    dh_sem,
    back_sem,
    pair_sem,
    gx_sem,
    xy_sem,
    xz_sem,
    xa_sem,
    zz_sem,
    zy_sem,
    zx_sem,
    za_sem,
):
    nz, nx, ny = sizes
    n_dom, n_snap = nz * nx, 2 * ny
    rows, width = x_ref.shape
    halo = n_dom * 8
    table = rows + halo
    block = rows // n_snap
    cols = 2 * width // nx
    chalf = cols // 2
    wrows = width // n_snap
    zc = min(4, nz)
    zrows, zcols = wrows // (nz // zc), width // zc
    scale = (width // HEADS) ** -0.5
    scale_bf = jnp.asarray(scale, BF)
    pairs = HEADS // 2

    loads = {
        "send": (send_hbm, send_ref),
        "x": (x_hbm, x_ref),
        "ws": (ws_hbm, ws_ref),
        "nbr": (nbr_hbm, nbr_ref),
        "rel": (rel_hbm, rel_ref),
        "rb": (rb_hbm, rb_ref),
        "act": (act_hbm, act_ref),
        "pos": (pos_hbm, pos_ref),
        "ct": (ct_hbm, ct_ref),
        "wt": (wt_hbm, wt_ref),
    }
    order = list(loads)

    def input_copy(name):
        return pltpu.make_async_copy(*loads[name], in_sem.at[order.index(name)])

    def arrive(name, load=True):
        input_copy(name).wait()
        return loads[name][1][...] if load else None

    for name in order:
        input_copy(name).start()

    me_d = lax.axis_index("dom")
    me_s = lax.axis_index("snap")
    me_z, me_x = me_d // nx, lax.rem(me_d, nx)
    me_y, me_c = me_s // 2, lax.rem(me_s, 2)
    partner = {"snap": me_s + 1 - 2 * me_c}

    barrier = pltpu.get_barrier_semaphore()

    dom, dom_at = (nz, nx), (me_z, me_x)
    snap, snap_at = (ny, -2), (me_y, me_c)
    to_dom = lambda p: {"dom": p}
    to_snap = lambda p: {"snap": p}
    to_x = lambda p: {"dom": me_z * nx + p}
    to_z = lambda p: {"dom": p * nx + me_x}
    to_y = lambda p: {"snap": p * 2 + me_c}
    for shift in far_first(dom):
        peer = to_dom(moved(dom_at, shift, dom))
        pl.semaphore_signal(barrier, inc=1, device_id=peer, device_id_type=MESH)
    for shift in far_first(snap):
        peer = to_snap(moved(snap_at, shift, snap))
        pl.semaphore_signal(barrier, inc=1, device_id=peer, device_id_type=MESH)

    halo_x = Exchange(dom, dom_at, to_dom, lambda p: halo_s.at[p], halo_r, halo_sem)
    hid_x = Exchange(snap, snap_at, to_snap, lambda p: hid_s.at[p], hid_r, hid_sem)
    dh_x = Exchange(snap, snap_at, to_snap, lambda p: dh_s.at[p], dh_r, dh_sem)
    back_x = Exchange(dom, dom_at, to_dom, lambda p: back_s.at[p], back_r, back_sem)
    def halved(dims, me, device_of, src, dst, sems):
        return [
            Exchange(dims, me, device_of, lambda p, g=g: src(g, p), dst.at[g], sems.at[g])
            for g in range(2)
        ]

    px_x = halved((nx,), (me_x,), to_x, lambda g, p: gx_s.at[g, p], gx_r, gx_sem)
    py_x = halved((ny,), (me_y,), to_y, lambda g, p: xy_s.at[g, p], xy_r, xy_sem)
    pz_x = halved((nz,), (me_z,), to_z, lambda g, p: xz_r.at[g, me_z], xz_r, xz_sem)
    pa_x = halved((nx,), (me_x,), to_x, lambda g, p: xa_r.at[g, me_x], xa_r, xa_sem)
    qz_x = Exchange((nz,), (me_z,), to_z, lambda p: zz_s.at[p], zz_r, zz_sem)
    qy_x = Exchange((ny,), (me_y,), to_y, lambda p: zy_s.at[p], zy_r, zy_sem)
    qx_x = Exchange((nx,), (me_x,), to_x, lambda p: zx_r.at[me_x], zx_r, zx_sem)
    qa_x = Exchange((nz,), (me_z,), to_z, lambda p: za_r.at[me_z], za_r, za_sem)
    pair = [
        copy_to(zt.at[:, 1 - me_c], zt_p, pair_sem.at[0, 3], pair_sem.at[1, 3], partner)
    ] + [
        copy_to(dt.at[i], dt_p.at[i], pair_sem.at[0, i], pair_sem.at[1, i], partner)
        for i in range(3)
    ]

    send_f = arrive("send").astype(F32).astype(BF)
    spread = (iota((n_dom, halo), 1) // 8 == iota((n_dom, halo), 0)).astype(F32).astype(BF)
    wide = mm(send_f, spread)
    picked = jnp.where(lax.rem(iota((8, halo), 1), 8) == iota((8, halo), 0), wide, 0.0)
    send_row = jnp.sum(picked, axis=0, keepdims=True)
    pick_t = (iota((rows, halo), 0).astype(F32) == send_row).astype(F32)
    pick = pick_t.T.astype(BF)
    x_val = arrive("x")
    tiles = mm(pick, x_val)
    halo_s[...] = tiles.reshape(n_dom, 8, width).astype(BF)

    pl.semaphore_wait(barrier, n_dom + n_snap - 2)
    halo_x.start()
    halo_r[me_d] = halo_s[me_d]

    half = iota((rows, 128), 1) < 64

    def stack(value):
        zero = jnp.zeros_like(value)
        return jnp.concatenate(
            [jnp.where(half, value, zero), jnp.where(half, zero, value)], axis=0
        )

    w_v = pl.ds(2 * width, width)
    arrive("ws", load=False)
    own = mm(x_val, ws_ref[...]).astype(BF)
    ktab[0:rows, :] = own[:, width : 2 * width]
    vtab[0:rows, :] = own[:, 2 * width :]
    for p in range(pairs):
        qst[p] = stack(own[:, 128 * p : 128 * p + 128] * scale_bf)
    wvt[...] = ws_ref[:, w_v].T
    vt[:, 0:rows] = mm_nt(wvt[...], x_val).astype(BF)

    nbr = arrive("nbr").astype(F32)
    slots = nbr.shape[0]
    place = (1 << (4 * arrive("rel"))).astype(F32)
    row_t = iota((table, rows), 0).astype(F32)
    packed = jnp.zeros((table, rows), F32)
    for k in range(slots):
        packed += jnp.where(row_t == nbr[k : k + 1, :], place[k : k + 1, :], 0.0)
    packed = packed.astype(jnp.int32)
    counts = [((packed >> (4 * r)) & 15).astype(F32) for r in range(4)]
    eb = jnp.exp(arrive("rb"))
    for h in range(HEADS):
        total = counts[0] * eb[0:1, h : h + 1]
        for r in range(1, 4):
            total += counts[r] * eb[r : r + 1, h : h + 1]
        cmat[h // 2, :, (h % 2) * rows : (h % 2) * rows + rows] = jnp.where(
            packed > 0, jnp.log(total), -1e30
        )

    row_i = iota((rows, rows), 0)
    col_i = iota((rows, rows), 1)
    act_f = arrive("act").astype(F32).astype(BF)
    over = (iota((n_snap, rows), 1) // block == iota((n_snap, rows), 0)).astype(F32)
    act_w = mm(act_f, over.astype(BF))
    act_own = lax.rem(iota((block, rows), 1), block) == iota((block, rows), 0)
    act_row = jnp.sum(jnp.where(act_own, act_w, 0.0), axis=0, keepdims=True)
    same = lax.rem(row_i, block) == lax.rem(col_i, block)
    earlier = jnp.where(col_i // block <= row_i // block, act_row, 0.0)
    allowed = jnp.where(row_i == col_i, 1.0, jnp.where(same, earlier, 0.0)).T
    allow[:, 0:rows] = allowed
    allow[:, rows:] = allowed
    step_1h = (iota((rows, n_snap), 0) // block == iota((rows, n_snap), 1)).astype(F32)
    pos_rows[...] = mm(step_1h.astype(BF), arrive("pos"))
    ct_f = arrive("ct").astype(F32).reshape(rows, width)
    ct = ct_f.astype(BF)
    for p in range(pairs):
        cts[p] = stack(ct[:, 128 * p : 128 * p + 128])

    halo_x.wait_recv()
    halo_rows = halo_r[...].astype(F32).reshape(halo, width).astype(BF)
    ktab[rows:, :] = mm(halo_rows, ws_ref[:, width : 2 * width]).astype(BF)
    vt[:, rows:] = mm_nt(wvt[...], halo_rows).astype(BF)

    for p in range(pairs):
        attn[p] = mm_nt(ktab[:, 128 * p : 128 * p + 128], qst[p])
    for p in range(pairs):
        score = attn[p] + cmat[p]
        e = jnp.exp(score - jnp.max(score, axis=0, keepdims=True))
        w = e * (1.0 / jnp.sum(e, axis=0, keepdims=True))
        attn[p] = w
        attn_b[p] = w.astype(BF)
    for p in range(pairs):
        o = mm(vt[128 * p : 128 * p + 128, :], attn_b[p])
        agg_t[128 * p : 128 * p + 64, :] = o[0:64, 0:rows]
        agg_t[128 * p + 64 : 128 * p + 128, :] = o[64:128, rows:]
    agg = agg_t[...].T
    hidden = x_val.astype(F32) + jnp.where(agg > 0, agg, jnp.exp(jnp.minimum(agg, 0.0)) - 1.0)
    hid_s[...] = hidden.reshape(n_snap, block, width).astype(BF)
    hid_x.start()
    hid_r[me_s] = hid_s[me_s]
    slope[...] = jnp.where(agg > 0, 1.0, jnp.exp(jnp.minimum(agg, 0.0)))
    vtab[rows:, :] = mm(halo_rows, ws_ref[:, w_v]).astype(BF)
    ktt[...] = ktab[...].T
    arrive("wt", load=False)
    halo_x.wait_send()

    hid_x.wait_recv()
    z_f = hid_r[...].astype(F32).reshape(rows, width) + pos_rows[...]
    z = z_f.astype(BF)
    tp[...] = mm(z, wt_ref[...]).astype(BF)
    zt[...] = z_f.T.astype(BF).reshape(ny, 2, width // n_snap, rows)
    pair[0].start()
    for p in range(pairs):
        tqs[p] = stack(tp[:, 128 * p : 128 * p + 128] * scale_bf)
        t_s[p] = mm_nt(tp[:, width + 128 * p : width + 128 * p + 128], tqs[p])
        t_d[p] = mm_nt(tp[:, 2 * width + 128 * p : 2 * width + 128 * p + 128], cts[p])
    for p in range(pairs):
        score = jnp.where(allow[...] > 0, t_s[p], -1e30)
        e = jnp.exp(score - jnp.max(score, axis=0, keepdims=True))
        w = e * (1.0 / jnp.sum(e, axis=0, keepdims=True))
        t = w * t_d[p]
        t_w[p] = w.astype(BF)
        t_b[p] = (t - w * jnp.sum(t, axis=0, keepdims=True)).astype(BF)
    for p in range(pairs):
        dt[2, :, 128 * p : 128 * p + 128] = mm(t_w[p], cts[p]).astype(BF)
    pair[3].start()
    for p in range(pairs):
        dt[1, :, 128 * p : 128 * p + 128] = mm(t_b[p], tqs[p]).astype(BF)
    pair[2].start()
    for p in range(pairs):
        at = 128 * p
        dq = mm_tn(t_b[p], tp[:, width + at : width + at + 128]) * scale
        dt[0, :, at : at + 128] = jnp.where(half, dq[0:rows], dq[rows:]).astype(BF)
    pair[1].start()

    d_z = ct_f
    for i in range(3):
        d_z += mm_nt(dt[i], wt_ref[:, width * i : width * i + width])
    dh_s[...] = d_z.reshape(n_snap, block, width).astype(BF)
    dh_x.start()
    dh_r[me_s] = dh_s[me_s]

    pair[0].wait_recv()
    z_both = jnp.concatenate(
        [zt[:, me_c].reshape(width // 2, rows), zt_p[...].reshape(width // 2, rows)], axis=1
    )
    pair[3].wait_recv()
    product = mm(z_both, jnp.concatenate([dt[2], dt_p[2]], axis=0)).reshape(ny, wrows, width)
    for i in range(nz):
        r, c = i // zc * zrows, i % zc * zcols
        zz_s[i] = product[:, r : r + zrows, c : c + zcols].astype(BF)
    qz_x.start()
    zz_r[me_z] = zz_s[me_z]
    pair[2].wait_recv()
    pair[1].wait_recv()
    for i in range(nx):
        part, c = i * cols // width, i * cols % width
        d_both = jnp.concatenate([dt[part, :, c : c + cols], dt_p[part, :, c : c + cols]], axis=0)
        prod = mm(z_both, d_both).astype(BF)
        gx_s[0, i] = prod[:, :chalf]
        gx_s[1, i] = prod[:, chalf:]
    px_x[0].start()
    px_x[1].start()

    hid_x.wait_send()
    dh_x.wait_recv()
    dh_f = dh_r[...].astype(F32).reshape(rows, width)
    d_agg = (dh_f * slope[...]).astype(BF)
    for p in range(pairs):
        das[p] = stack(d_agg[:, 128 * p : 128 * p + 128])
        d_att[p] = mm_nt(vtab[:, 128 * p : 128 * p + 128], das[p])
    for p in range(pairs):
        w = attn[p]
        t = w * d_att[p]
        d_sc[p] = (t - w * jnp.sum(t, axis=0, keepdims=True)).astype(BF)
    for p in range(pairs):
        at = 128 * p
        dkv[rows:, at : at + 128] = mm(d_sc[p, rows:, :], qst[p]).astype(BF)
        dkv[rows:, width + at : width + at + 128] = mm(attn_b[p, rows:, :], das[p]).astype(BF)

    d_halo = mm_nt(dkv[rows:, :], ws_ref[:, width:])
    back_s[...] = d_halo.reshape(n_dom, 8, width).astype(BF)
    back_x.start()
    back_r[me_d] = back_s[me_d]

    def total_of(ref, count):
        total = ref[0].astype(F32)
        for i in range(1, count):
            total += ref[i].astype(F32)
        return total

    px_x[0].wait_recv()
    total = gx_s[0, me_x].astype(F32)
    for i in range(1, nx):
        total += gx_r[0, lax.rem(me_x + i, nx)].astype(F32)
    xy_s[0] = total.astype(BF).reshape(ny, wrows, chalf)
    py_x[0].start()
    xy_r[0, me_y] = xy_s[0, me_y]

    qz_x.wait_recv()
    zy_s[...] = total_of(zz_r, nz).astype(BF)
    qy_x.start()
    zy_r[me_y] = zy_s[me_y]

    px_x[1].wait_recv()
    total = gx_s[1, me_x].astype(F32)
    for i in range(1, nx):
        total += gx_r[1, lax.rem(me_x + i, nx)].astype(F32)
    xy_s[1] = total.astype(BF).reshape(ny, wrows, chalf)
    py_x[1].start()
    xy_r[1, me_y] = xy_s[1, me_y]

    for p in range(pairs):
        at = 128 * p
        dkv[0:rows, at : at + 128] = mm(d_sc[p, 0:rows, :], qst[p]).astype(BF)
        dkv[0:rows, width + at : width + at + 128] = mm(attn_b[p, 0:rows, :], das[p]).astype(BF)
        o = mm(ktt[at : at + 128, :], d_sc[p]) * scale
        agg_t[at : at + 64, :] = o[0:64, 0:rows]
        agg_t[at + 64 : at + 128, :] = o[64:128, rows:]
    dq = agg_t[...].T.astype(BF)
    d_own = dh_f + mm_nt(dq, ws_ref[:, :width]) + mm_nt(dkv[0:rows, :], ws_ref[:, width:])
    dh_x.wait_send()
    px_x[0].wait_send()
    px_x[1].wait_send()
    for copy in pair:
        copy.wait_send()

    py_x[0].wait_recv()
    xz_r[0, me_z] = total_of(xy_r.at[0], ny).astype(BF)
    pz_x[0].start()
    qy_x.wait_recv()
    zx_r[me_x] = total_of(zy_r, ny).astype(BF)
    qx_x.start()
    qy_x.wait_send()

    py_x[1].wait_recv()
    xz_r[1, me_z] = total_of(xy_r.at[1], ny).astype(BF)
    pz_x[1].start()
    back_x.wait_recv()
    came = back_r[...].astype(F32).reshape(halo, width).astype(BF)
    out_ref[...] = (d_own + mm(pick_t.astype(BF), came)).astype(BF)
    save_out = pltpu.make_async_copy(out_ref, out_hbm, out_sem.at[0])
    save_out.start()

    qx_x.wait_recv()
    za_r[me_z] = total_of(zx_r, nx).astype(BF)
    qa_x.start()
    pz_x[0].wait_recv()
    xa_r[0, me_x] = total_of(xz_r.at[0], nz).astype(BF)
    pa_x[0].start()
    pz_x[1].wait_recv()
    xa_r[1, me_x] = total_of(xz_r.at[1], nz).astype(BF)
    pa_x[1].start()
    for exchange in (back_x, qz_x, qx_x, *py_x, *pz_x):
        exchange.wait_send()
    qa_x.wait_recv()
    for i in range(nz):
        r, c = i // zc * zrows, 2 * width + i % zc * zcols
        gw_ref[r : r + zrows, c : c + zcols] = za_r[i].astype(F32)
    for g in range(2):
        pa_x[g].wait_recv()
        for i in range(nx):
            c = cols * i + chalf * g
            gw_ref[:, c : c + chalf] = xa_r[g, i].astype(F32)
    save_gw = pltpu.make_async_copy(gw_ref, gw_hbm, out_sem.at[1])
    save_gw.start()
    pa_x[0].wait_send()
    pa_x[1].wait_send()
    qa_x.wait_send()
    save_out.wait()
    save_gw.wait()


def emit(grad_in, gw_in, grad_out, gw_out, sem):
    first = pltpu.make_async_copy(gw_in, gw_out, sem.at[0])
    second = pltpu.make_async_copy(grad_in, grad_out, sem.at[1])
    first.start()
    second.start()
    first.wait()
    second.wait()


def per_device(
    feat, w_struct, w_temp, pos_embed, rel_bias, nbr, rel_type, send_idx, active, cotangent
):
    x = feat[0]
    rows, width = x.shape
    n_dom, n_snap = lax.axis_size("dom"), lax.axis_size("snap")
    nz, nx = GRID[n_dom]
    ny = n_snap // 2
    halo = n_dom * 8
    table = rows + halo
    block = rows // n_snap
    cols = 2 * width // nx
    chalf = cols // 2
    wrows = width // n_snap
    zc = min(4, nz)
    zrows, zcols = wrows // (nz // zc), width // zc
    vm = pltpu.VMEM
    dma = pltpu.SemaphoreType.DMA
    arrays = (
        x,
        w_struct,
        w_temp,
        pos_embed,
        rel_bias,
        nbr[0].T,
        rel_type[0].T,
        send_idx[0, 0].T,
        active.T,
        cotangent,
    )
    pairs = HEADS // 2
    scratch = [vm(a.shape, a.dtype) for a in arrays] + [
        dma((len(arrays),)),
        vm((rows, width), BF),
        vm((wrows, 3 * width), F32),
        dma((2,)),
        vm((n_dom, 8, width), BF),
        vm((n_dom, 8, width), BF),
        vm((n_snap, block, width), BF),
        vm((n_snap, block, width), BF),
        vm((n_snap, block, width), BF),
        vm((n_snap, block, width), BF),
        vm((n_dom, 8, width), BF),
        vm((n_dom, 8, width), BF),
        vm((ny, 2, wrows, rows), BF),
        vm((ny, wrows, rows), BF),
        vm((3, rows, width), BF),
        vm((3, rows, width), BF),
        vm((2, nx, width // 2, chalf), BF),
        vm((2, nx, width // 2, chalf), BF),
        vm((2, ny, wrows, chalf), BF),
        vm((2, ny, wrows, chalf), BF),
        vm((2, nz, wrows, chalf), BF),
        vm((2, nx, wrows, chalf), BF),
        vm((nz, ny, zrows, zcols), BF),
        vm((nz, ny, zrows, zcols), BF),
        vm((ny, zrows, zcols), BF),
        vm((ny, zrows, zcols), BF),
        vm((nx, zrows, zcols), BF),
        vm((nz, zrows, zcols), BF),
        vm((pairs, 2 * rows, 128), BF),
        vm((table, width), BF),
        vm((table, width), BF),
        vm((width, width), BF),
        vm((width, table), BF),
        vm((width, table), BF),
        vm((pairs, table, 2 * rows), F32),
        vm((pairs, table, 2 * rows), F32),
        vm((pairs, table, 2 * rows), BF),
        vm((pairs, table, 2 * rows), F32),
        vm((pairs, table, 2 * rows), BF),
        vm((pairs, 2 * rows, 128), BF),
        vm((width, rows), F32),
        vm((rows, width), F32),
        vm((table, 2 * width), BF),
        vm((rows, 2 * rows), F32),
        vm((rows, width), F32),
        vm((pairs, 2 * rows, 128), BF),
        vm((rows, 3 * width), BF),
        vm((pairs, 2 * rows, 128), BF),
        vm((pairs, rows, 2 * rows), F32),
        vm((pairs, rows, 2 * rows), F32),
        vm((pairs, rows, 2 * rows), BF),
        vm((pairs, rows, 2 * rows), BF),
        dma((2,)),
        dma((2,)),
        dma((2,)),
        dma((2,)),
        dma((2, 4)),
        dma((2, 2)),
        dma((2, 2)),
        dma((2, 2)),
        dma((2, 2)),
        dma((2,)),
        dma((2,)),
        dma((2,)),
        dma((2,)),
    ]
    in_any = pl.BlockSpec(memory_space=pl.ANY)
    grad, gw = pl.pallas_call(
        functools.partial(kernel, (nz, nx, ny)),
        out_shape=(
            jax.ShapeDtypeStruct((rows, width), BF),
            jax.ShapeDtypeStruct((wrows, 3 * width), F32),
        ),
        in_specs=[in_any] * len(arrays),
        out_specs=(in_any,) * 2,
        scratch_shapes=scratch,
        compiler_params=pltpu.CompilerParams(
            collective_id=0, has_side_effects=True, vmem_limit_bytes=48 * 2**20
        ),
        name="step",
    )(*[pltpu.with_memory_space_constraint(a, pltpu.HBM) for a in arrays])
    grad, gw = pl.pallas_call(
        emit,
        out_shape=(
            jax.ShapeDtypeStruct(grad.shape, BF),
            jax.ShapeDtypeStruct(gw.shape, F32),
        ),
        in_specs=[in_any] * 2,
        out_specs=(in_any,) * 2,
        scratch_shapes=[dma((2,))],
        compiler_params=pltpu.CompilerParams(vmem_limit_bytes=4 * 2**20),
        name="emit",
    )(grad, gw)
    return (grad[None], gw)


def solution(mesh):
    return jax.shard_map(
        per_device,
        mesh=mesh,
        in_specs=(
            P("snap", "dom", None),
            P(),
            P(),
            P(),
            P(),
            P("snap", "dom", None),
            P("snap", "dom", None),
            P("snap", "dom", None, None),
            P(None, ("dom", "snap")),
            P(None, ("dom", "snap"), None),
        ),
        out_specs=(P("snap", "dom", None), P("snap", None)),
        check_vma=False,
    )
```

```python
import functools

import jax
import jax.numpy as jnp
from jax import lax
from jax.experimental import pallas as pl
from jax.experimental.pallas import tpu as pltpu
from jax.sharding import PartitionSpec as P

HEADS = 8
MESH = pl.DeviceIdType.MESH
BF = jnp.bfloat16
F32 = jnp.float32
GRID = {32: (8, 4), 4: (2, 2), 8: (2, 4)}


def mm(a, b):
    return jnp.dot(a, b, preferred_element_type=F32)


def mm_nt(a, b):
    return lax.dot_general(a, b, (((1,), (1,)), ((), ())), preferred_element_type=F32)


def mm_tn(a, b):
    return lax.dot_general(a, b, (((0,), (0,)), ((), ())), preferred_element_type=F32)


def iota(shape, axis):
    return lax.broadcasted_iota(jnp.int32, shape, axis)


def where_bf(mask, value):
    return jnp.where(mask, value, jnp.zeros_like(value))


def copy_to(src, dst, send_sem, recv_sem, device):
    return pltpu.make_async_remote_copy(
        src_ref=src,
        dst_ref=dst,
        send_sem=send_sem,
        recv_sem=recv_sem,
        device_id=device,
        device_id_type=MESH,
    )


def ring(shift, size):
    return min(shift, size - shift)


def far_first(dims):
    shifts = [()]
    for size in dims:
        shifts = [s + (i,) for s in shifts for i in range(abs(size))]
    hops = lambda s: sum(ring(i, n) if n > 0 else 0.1 * i for i, n in zip(s, dims))
    return sorted((s for s in shifts if any(s)), key=lambda s: -hops(s))


def moved(me, shift, dims):
    index = 0
    for at, step, size in zip(me, shift, dims):
        index = index * abs(size) + (lax.rem(at + step, abs(size)) if step else at)
    return index


class Exchange:
    def __init__(self, dims, me, device_of, src, dst, sems):
        self.dims, self.at, self.device_of = dims, me, device_of
        self.shifts = far_first(dims)
        self.me = moved(me, (0,) * len(dims), dims)
        self.count = len(self.shifts) + 1
        self.src, self.dst, self.send, self.recv = src, dst, sems.at[0], sems.at[1]

    def start(self):
        for shift in self.shifts:
            peer = moved(self.at, shift, self.dims)
            copy_to(
                self.src(peer),
                self.dst.at[self.me],
                self.send,
                self.recv,
                self.device_of(peer),
            ).start()

    def all_copies(self):
        others = self.dst.at[pl.ds(0, self.count - 1)]
        peer = moved(self.at, self.shifts[-1], self.dims)
        return copy_to(others, others, self.send, self.recv, self.device_of(peer))

    def wait_recv(self):
        if self.count > 1:
            self.all_copies().wait_recv()

    def wait_send(self):
        if self.count > 1:
            self.all_copies().wait_send()


def kernel(
    sizes,
    x_hbm,
    ws_hbm,
    wt_hbm,
    pos_hbm,
    rb_hbm,
    nbr_hbm,
    rel_hbm,
    send_hbm,
    act_hbm,
    ct_hbm,
    out_ref,
    gw_ref,
    x_ref,
    ws_ref,
    wt_ref,
    pos_ref,
    rb_ref,
    nbr_ref,
    rel_ref,
    send_ref,
    act_ref,
    ct_ref,
    in_sem,
    halo_s,
    halo_r,
    hid_s,
    hid_r,
    dh_s,
    dh_r,
    back_s,
    back_r,
    zt,
    zt_p,
    dt,
    dt_p,
    gx_s,
    gx_r,
    xy_s,
    xy_r,
    xz_r,
    xa_r,
    zz_s,
    zz_r,
    zy_s,
    zy_r,
    zx_r,
    za_r,
    qst,
    ktab,
    vtab,
    wvt,
    vt,
    ktt,
    cmat,
    attn,
    attn_b,
    d_att,
    d_sc,
    das,
    agg_t,
    slope,
    dkv,
    allow,
    pos_rows,
    cts,
    tp,
    tqs,
    t_w,
    t_b,
    halo_sem,
    hid_sem,
    dh_sem,
    back_sem,
    pair_sem,
    gx_sem,
    xy_sem,
    xz_sem,
    xa_sem,
    zz_sem,
    zy_sem,
    zx_sem,
    za_sem,
):
    nz, nx, ny = sizes
    n_dom, n_snap = nz * nx, 2 * ny
    rows, width = x_ref.shape
    halo = n_dom * 8
    table = rows + halo
    block = rows // n_snap
    cols = 2 * width // nx
    chalf = cols // 2
    wrows = width // n_snap
    zc = min(4, nz)
    zrows, zcols = wrows // (nz // zc), width // zc
    scale = (width // HEADS) ** -0.5
    scale_bf = jnp.asarray(scale, BF)
    pairs = HEADS // 2

    loads = {
        "send": (send_hbm, send_ref),
        "x": (x_hbm, x_ref),
        "ws": (ws_hbm, ws_ref),
        "nbr": (nbr_hbm, nbr_ref),
        "rel": (rel_hbm, rel_ref),
        "rb": (rb_hbm, rb_ref),
        "act": (act_hbm, act_ref),
        "pos": (pos_hbm, pos_ref),
        "ct": (ct_hbm, ct_ref),
        "wt": (wt_hbm, wt_ref),
    }
    order = list(loads)

    def input_copy(name):
        return pltpu.make_async_copy(*loads[name], in_sem.at[order.index(name)])

    def arrive(name, load=True):
        input_copy(name).wait()
        return loads[name][1][...] if load else None

    for name in order:
        input_copy(name).start()

    me_d = lax.axis_index("dom")
    me_s = lax.axis_index("snap")
    me_z, me_x = me_d // nx, lax.rem(me_d, nx)
    me_y, me_c = me_s // 2, lax.rem(me_s, 2)
    partner = {"snap": me_s + 1 - 2 * me_c}

    barrier = pltpu.get_barrier_semaphore()

    dom, dom_at = (nz, nx), (me_z, me_x)
    snap, snap_at = (ny, -2), (me_y, me_c)
    to_dom = lambda p: {"dom": p}
    to_snap = lambda p: {"snap": p}
    to_x = lambda p: {"dom": me_z * nx + p}
    to_z = lambda p: {"dom": p * nx + me_x}
    to_y = lambda p: {"snap": p * 2 + me_c}
    for shift in far_first(dom):
        peer = to_dom(moved(dom_at, shift, dom))
        pl.semaphore_signal(barrier, inc=1, device_id=peer, device_id_type=MESH)
    for shift in far_first(snap):
        peer = to_snap(moved(snap_at, shift, snap))
        pl.semaphore_signal(barrier, inc=1, device_id=peer, device_id_type=MESH)

    halo_x = Exchange(dom, dom_at, to_dom, lambda p: halo_s.at[p], halo_r, halo_sem)
    hid_x = Exchange(snap, snap_at, to_snap, lambda p: hid_s.at[p], hid_r, hid_sem)
    dh_x = Exchange(snap, snap_at, to_snap, lambda p: dh_s.at[p], dh_r, dh_sem)
    back_x = Exchange(dom, dom_at, to_dom, lambda p: back_s.at[p], back_r, back_sem)
    def halved(dims, me, device_of, src, dst, sems):
        return [
            Exchange(dims, me, device_of, lambda p, g=g: src(g, p), dst.at[g], sems.at[g])
            for g in range(2)
        ]

    px_x = halved((nx,), (me_x,), to_x, lambda g, p: gx_s.at[g, p], gx_r, gx_sem)
    py_x = halved((ny,), (me_y,), to_y, lambda g, p: xy_s.at[g, p], xy_r, xy_sem)
    pz_x = halved((nz,), (me_z,), to_z, lambda g, p: xz_r.at[g, me_z], xz_r, xz_sem)
    pa_x = halved((nx,), (me_x,), to_x, lambda g, p: xa_r.at[g, me_x], xa_r, xa_sem)
    qz_x = Exchange((nz,), (me_z,), to_z, lambda p: zz_s.at[p], zz_r, zz_sem)
    qy_x = Exchange((ny,), (me_y,), to_y, lambda p: zy_s.at[p], zy_r, zy_sem)
    qx_x = Exchange((nx,), (me_x,), to_x, lambda p: zx_r.at[me_x], zx_r, zx_sem)
    qa_x = Exchange((nz,), (me_z,), to_z, lambda p: za_r.at[me_z], za_r, za_sem)
    pair = [
        copy_to(zt.at[:, 1 - me_c], zt_p, pair_sem.at[0, 3], pair_sem.at[1, 3], partner)
    ] + [
        copy_to(dt.at[i], dt_p.at[i], pair_sem.at[0, i], pair_sem.at[1, i], partner)
        for i in range(3)
    ]

    send_f = arrive("send").astype(F32).astype(BF)
    spread = (iota((n_dom, halo), 1) // 8 == iota((n_dom, halo), 0)).astype(F32).astype(BF)
    wide = mm(send_f, spread)
    picked = jnp.where(lax.rem(iota((8, halo), 1), 8) == iota((8, halo), 0), wide, 0.0)
    send_row = jnp.sum(picked, axis=0, keepdims=True)
    pick_t = (iota((rows, halo), 0).astype(F32) == send_row).astype(F32)
    pick = pick_t.T.astype(BF)
    x_val = arrive("x")
    tiles = mm(pick, x_val)
    halo_s[...] = tiles.reshape(n_dom, 8, width).astype(BF)

    pl.semaphore_wait(barrier, n_dom + n_snap - 2)
    halo_x.start()
    halo_r[me_d] = halo_s[me_d]

    half = iota((rows, 128), 1) < 64

    def stack(value):
        zero = jnp.zeros_like(value)
        return jnp.concatenate(
            [jnp.where(half, value, zero), jnp.where(half, zero, value)], axis=0
        )

    w_v = pl.ds(2 * width, width)
    arrive("ws", load=False)
    own = mm(x_val, ws_ref[...]).astype(BF)
    ktab[0:rows, :] = own[:, width : 2 * width]
    vtab[0:rows, :] = own[:, 2 * width :]
    for p in range(pairs):
        qst[p] = stack(own[:, 128 * p : 128 * p + 128] * scale_bf)
    wvt[...] = ws_ref[:, w_v].T
    vt[:, 0:rows] = mm_nt(wvt[...], x_val).astype(BF)

    nbr = arrive("nbr").astype(F32)
    slots = nbr.shape[0]
    place = (1 << (4 * arrive("rel"))).astype(F32)
    row_t = iota((table, rows), 0).astype(F32)
    packed = jnp.zeros((table, rows), F32)
    for k in range(slots):
        packed += jnp.where(row_t == nbr[k : k + 1, :], place[k : k + 1, :], 0.0)
    packed = packed.astype(jnp.int32)
    counts = [((packed >> (4 * r)) & 15).astype(F32) for r in range(4)]
    eb = jnp.exp(arrive("rb"))
    for h in range(HEADS):
        total = counts[0] * eb[0:1, h : h + 1]
        for r in range(1, 4):
            total += counts[r] * eb[r : r + 1, h : h + 1]
        cmat[h // 2, :, (h % 2) * rows : (h % 2) * rows + rows] = jnp.where(
            packed > 0, jnp.log(total), -1e30
        )

    row_i = iota((rows, rows), 0)
    col_i = iota((rows, rows), 1)
    act_f = arrive("act").astype(F32).astype(BF)
    over = (iota((n_snap, rows), 1) // block == iota((n_snap, rows), 0)).astype(F32)
    act_w = mm(act_f, over.astype(BF))
    act_own = lax.rem(iota((block, rows), 1), block) == iota((block, rows), 0)
    act_row = jnp.sum(jnp.where(act_own, act_w, 0.0), axis=0, keepdims=True)
    same = lax.rem(row_i, block) == lax.rem(col_i, block)
    earlier = jnp.where(col_i // block <= row_i // block, act_row, 0.0)
    allowed = jnp.where(row_i == col_i, 1.0, jnp.where(same, earlier, 0.0)).T
    allowed = jnp.where(allowed > 0, 0.0, -1e30)
    allow[:, 0:rows] = allowed
    allow[:, rows:] = allowed
    step_1h = (iota((rows, n_snap), 0) // block == iota((rows, n_snap), 1)).astype(F32)
    pos_rows[...] = mm(step_1h.astype(BF), arrive("pos"))
    ct_f = arrive("ct").astype(F32).reshape(rows, width)
    ct = ct_f.astype(BF)
    for p in range(pairs):
        cts[p] = stack(ct[:, 128 * p : 128 * p + 128])

    halo_x.wait_recv()
    halo_rows = halo_r[...].astype(F32).reshape(halo, width).astype(BF)
    ktab[rows:, :] = mm(halo_rows, ws_ref[:, width : 2 * width]).astype(BF)
    vt[:, rows:] = mm_nt(wvt[...], halo_rows).astype(BF)

    for p in range(pairs):
        attn[p] = mm_nt(ktab[:, 128 * p : 128 * p + 128], qst[p])
    for p in range(pairs):
        score = attn[p] + cmat[p]
        e = jnp.exp(score - jnp.max(score, axis=0, keepdims=True))
        w = e * (1.0 / jnp.sum(e, axis=0, keepdims=True))
        attn[p] = w
        attn_b[p] = w.astype(BF)
    for p in range(pairs):
        o = mm(vt[128 * p : 128 * p + 128, :], attn_b[p])
        agg_t[128 * p : 128 * p + 64, :] = o[0:64, 0:rows]
        agg_t[128 * p + 64 : 128 * p + 128, :] = o[64:128, rows:]
    agg = agg_t[...].T
    hidden = x_val.astype(F32) + jnp.where(agg > 0, agg, jnp.exp(jnp.minimum(agg, 0.0)) - 1.0)
    hid_s[...] = hidden.reshape(n_snap, block, width).astype(BF)
    hid_x.start()
    hid_r[me_s] = hid_s[me_s]
    slope[...] = jnp.where(agg > 0, 1.0, jnp.exp(jnp.minimum(agg, 0.0)))
    vtab[rows:, :] = mm(halo_rows, ws_ref[:, w_v]).astype(BF)
    ktt[...] = ktab[...].T
    arrive("wt", load=False)
    halo_x.wait_send()

    hid_x.wait_recv()
    z_f = hid_r[...].astype(F32).reshape(rows, width) + pos_rows[...]
    z = z_f.astype(BF)
    tp[...] = mm(z, wt_ref[...]).astype(BF)
    zt[...] = z_f.T.astype(BF).reshape(ny, 2, width // n_snap, rows)
    pair[0].start()
    for p in range(pairs):
        at = 128 * p
        tqs[p] = stack(tp[:, at : at + 128] * scale_bf)
        score = mm_nt(tp[:, width + at : width + at + 128], tqs[p]) + allow[...]
        d_w = mm_nt(tp[:, 2 * width + at : 2 * width + at + 128], cts[p])
        e = jnp.exp(score - jnp.max(score, axis=0, keepdims=True))
        w = e * (1.0 / jnp.sum(e, axis=0, keepdims=True))
        t = w * d_w
        t_w[p] = w.astype(BF)
        t_b[p] = (t - w * jnp.sum(t, axis=0, keepdims=True)).astype(BF)
    for p in range(pairs):
        dt[2, :, 128 * p : 128 * p + 128] = mm(t_w[p], cts[p]).astype(BF)
    pair[3].start()
    for p in range(pairs):
        dt[1, :, 128 * p : 128 * p + 128] = mm(t_b[p], tqs[p]).astype(BF)
    pair[2].start()
    for p in range(pairs):
        at = 128 * p
        dq = mm_tn(t_b[p], tp[:, width + at : width + at + 128]) * scale
        dt[0, :, at : at + 128] = jnp.where(half, dq[0:rows], dq[rows:]).astype(BF)
    pair[1].start()

    d_z = ct_f
    for i in range(3):
        d_z += mm_nt(dt[i], wt_ref[:, width * i : width * i + width])
    dh_s[...] = d_z.reshape(n_snap, block, width).astype(BF)
    dh_x.start()
    dh_r[me_s] = dh_s[me_s]

    pair[0].wait_recv()
    z_both = jnp.concatenate(
        [zt[:, me_c].reshape(width // 2, rows), zt_p[...].reshape(width // 2, rows)], axis=1
    )
    pair[3].wait_recv()
    product = mm(z_both, jnp.concatenate([dt[2], dt_p[2]], axis=0)).reshape(ny, wrows, width)
    for i in range(nz):
        r, c = i // zc * zrows, i % zc * zcols
        zz_s[i] = product[:, r : r + zrows, c : c + zcols].astype(BF)
    qz_x.start()
    zz_r[me_z] = zz_s[me_z]
    pair[2].wait_recv()
    pair[1].wait_recv()
    for i in range(nx):
        part, c = i * cols // width, i * cols % width
        d_both = jnp.concatenate([dt[part, :, c : c + cols], dt_p[part, :, c : c + cols]], axis=0)
        prod = mm(z_both, d_both).astype(BF)
        gx_s[0, i] = prod[:, :chalf]
        gx_s[1, i] = prod[:, chalf:]
    px_x[0].start()
    px_x[1].start()

    hid_x.wait_send()
    dh_x.wait_recv()
    dh_f = dh_r[...].astype(F32).reshape(rows, width)
    d_agg = (dh_f * slope[...]).astype(BF)
    for p in range(pairs):
        das[p] = stack(d_agg[:, 128 * p : 128 * p + 128])
        d_att[p] = mm_nt(vtab[:, 128 * p : 128 * p + 128], das[p])
    for p in range(pairs):
        w = attn[p]
        t = w * d_att[p]
        d_sc[p] = (t - w * jnp.sum(t, axis=0, keepdims=True)).astype(BF)
    for p in range(pairs):
        at = 128 * p
        dkv[rows:, at : at + 128] = mm(d_sc[p, rows:, :], qst[p]).astype(BF)
        dkv[rows:, width + at : width + at + 128] = mm(attn_b[p, rows:, :], das[p]).astype(BF)

    d_halo = mm_nt(dkv[rows:, :], ws_ref[:, width:])
    back_s[...] = d_halo.reshape(n_dom, 8, width).astype(BF)
    back_x.start()
    back_r[me_d] = back_s[me_d]

    def total_of(ref, count):
        total = ref[0].astype(F32)
        for i in range(1, count):
            total += ref[i].astype(F32)
        return total

    px_x[0].wait_recv()
    total = gx_s[0, me_x].astype(F32)
    for i in range(1, nx):
        total += gx_r[0, lax.rem(me_x + i, nx)].astype(F32)
    xy_s[0] = total.astype(BF).reshape(ny, wrows, chalf)
    py_x[0].start()
    xy_r[0, me_y] = xy_s[0, me_y]

    qz_x.wait_recv()
    zy_s[...] = total_of(zz_r, nz).astype(BF)
    qy_x.start()
    zy_r[me_y] = zy_s[me_y]

    px_x[1].wait_recv()
    total = gx_s[1, me_x].astype(F32)
    for i in range(1, nx):
        total += gx_r[1, lax.rem(me_x + i, nx)].astype(F32)
    xy_s[1] = total.astype(BF).reshape(ny, wrows, chalf)
    py_x[1].start()
    xy_r[1, me_y] = xy_s[1, me_y]

    for p in range(pairs):
        at = 128 * p
        dkv[0:rows, at : at + 128] = mm(d_sc[p, 0:rows, :], qst[p]).astype(BF)
        dkv[0:rows, width + at : width + at + 128] = mm(attn_b[p, 0:rows, :], das[p]).astype(BF)
        o = mm(ktt[at : at + 128, :], d_sc[p]) * scale
        agg_t[at : at + 64, :] = o[0:64, 0:rows]
        agg_t[at + 64 : at + 128, :] = o[64:128, rows:]
    dq = agg_t[...].T.astype(BF)
    d_own = dh_f + mm_nt(dq, ws_ref[:, :width]) + mm_nt(dkv[0:rows, :], ws_ref[:, width:])
    dh_x.wait_send()
    px_x[0].wait_send()
    px_x[1].wait_send()
    for copy in pair:
        copy.wait_send()

    py_x[0].wait_recv()
    xz_r[0, me_z] = total_of(xy_r.at[0], ny).astype(BF)
    pz_x[0].start()
    qy_x.wait_recv()
    zx_r[me_x] = total_of(zy_r, ny).astype(BF)
    qx_x.start()
    qy_x.wait_send()

    py_x[1].wait_recv()
    xz_r[1, me_z] = total_of(xy_r.at[1], ny).astype(BF)
    pz_x[1].start()
    back_x.wait_recv()
    came = back_r[...].astype(F32).reshape(halo, width).astype(BF)
    out_ref[...] = (d_own + mm(pick_t.astype(BF), came)).astype(BF)

    qx_x.wait_recv()
    za_r[me_z] = total_of(zx_r, nx).astype(BF)
    qa_x.start()
    pz_x[0].wait_recv()
    xa_r[0, me_x] = total_of(xz_r.at[0], nz).astype(BF)
    pa_x[0].start()
    pz_x[1].wait_recv()
    xa_r[1, me_x] = total_of(xz_r.at[1], nz).astype(BF)
    pa_x[1].start()
    for exchange in (back_x, qz_x, qx_x, *py_x, *pz_x):
        exchange.wait_send()
    qa_x.wait_recv()
    for i in range(nz):
        r, c = i // zc * zrows, 2 * width + i % zc * zcols
        gw_ref[r : r + zrows, c : c + zcols] = za_r[i].astype(F32)
    for g in range(2):
        pa_x[g].wait_recv()
        for i in range(nx):
            c = cols * i + chalf * g
            gw_ref[:, c : c + chalf] = xa_r[g, i].astype(F32)
    pa_x[0].wait_send()
    pa_x[1].wait_send()
    qa_x.wait_send()


def emit(grad_in, gw_in, grad_out, gw_out, sem):
    first = pltpu.make_async_copy(gw_in, gw_out, sem.at[0])
    second = pltpu.make_async_copy(grad_in, grad_out, sem.at[1])
    first.start()
    second.start()
    first.wait()
    second.wait()


def per_device(
    feat, w_struct, w_temp, pos_embed, rel_bias, nbr, rel_type, send_idx, active, cotangent
):
    x = feat[0]
    rows, width = x.shape
    n_dom, n_snap = lax.axis_size("dom"), lax.axis_size("snap")
    nz, nx = GRID[n_dom]
    ny = n_snap // 2
    halo = n_dom * 8
    table = rows + halo
    block = rows // n_snap
    cols = 2 * width // nx
    chalf = cols // 2
    wrows = width // n_snap
    zc = min(4, nz)
    zrows, zcols = wrows // (nz // zc), width // zc
    vm = pltpu.VMEM
    dma = pltpu.SemaphoreType.DMA
    arrays = (
        x,
        w_struct,
        w_temp,
        pos_embed,
        rel_bias,
        nbr[0].T,
        rel_type[0].T,
        send_idx[0, 0].T,
        active.T,
        cotangent,
    )
    pairs = HEADS // 2
    scratch = [vm(a.shape, a.dtype) for a in arrays] + [
        dma((len(arrays),)),
        vm((n_dom, 8, width), BF),
        vm((n_dom, 8, width), BF),
        vm((n_snap, block, width), BF),
        vm((n_snap, block, width), BF),
        vm((n_snap, block, width), BF),
        vm((n_snap, block, width), BF),
        vm((n_dom, 8, width), BF),
        vm((n_dom, 8, width), BF),
        vm((ny, 2, wrows, rows), BF),
        vm((ny, wrows, rows), BF),
        vm((3, rows, width), BF),
        vm((3, rows, width), BF),
        vm((2, nx, width // 2, chalf), BF),
        vm((2, nx, width // 2, chalf), BF),
        vm((2, ny, wrows, chalf), BF),
        vm((2, ny, wrows, chalf), BF),
        vm((2, nz, wrows, chalf), BF),
        vm((2, nx, wrows, chalf), BF),
        vm((nz, ny, zrows, zcols), BF),
        vm((nz, ny, zrows, zcols), BF),
        vm((ny, zrows, zcols), BF),
        vm((ny, zrows, zcols), BF),
        vm((nx, zrows, zcols), BF),
        vm((nz, zrows, zcols), BF),
        vm((pairs, 2 * rows, 128), BF),
        vm((table, width), BF),
        vm((table, width), BF),
        vm((width, width), BF),
        vm((width, table), BF),
        vm((width, table), BF),
        vm((pairs, table, 2 * rows), F32),
        vm((pairs, table, 2 * rows), F32),
        vm((pairs, table, 2 * rows), BF),
        vm((pairs, table, 2 * rows), F32),
        vm((pairs, table, 2 * rows), BF),
        vm((pairs, 2 * rows, 128), BF),
        vm((width, rows), F32),
        vm((rows, width), F32),
        vm((table, 2 * width), BF),
        vm((rows, 2 * rows), F32),
        vm((rows, width), F32),
        vm((pairs, 2 * rows, 128), BF),
        vm((rows, 3 * width), BF),
        vm((pairs, 2 * rows, 128), BF),
        vm((pairs, rows, 2 * rows), BF),
        vm((pairs, rows, 2 * rows), BF),
        dma((2,)),
        dma((2,)),
        dma((2,)),
        dma((2,)),
        dma((2, 4)),
        dma((2, 2)),
        dma((2, 2)),
        dma((2, 2)),
        dma((2, 2)),
        dma((2,)),
        dma((2,)),
        dma((2,)),
        dma((2,)),
    ]
    in_any = pl.BlockSpec(memory_space=pl.ANY)
    grad, gw = pl.pallas_call(
        functools.partial(kernel, (nz, nx, ny)),
        out_shape=(
            jax.ShapeDtypeStruct((rows, width), BF),
            jax.ShapeDtypeStruct((wrows, 3 * width), F32),
        ),
        in_specs=[in_any] * len(arrays),
        out_specs=(pl.BlockSpec(memory_space=pltpu.VMEM),) * 2,
        scratch_shapes=scratch,
        compiler_params=pltpu.CompilerParams(
            collective_id=0, has_side_effects=True, vmem_limit_bytes=48 * 2**20
        ),
        name="step",
    )(*[pltpu.with_memory_space_constraint(a, pltpu.HBM) for a in arrays])
    grad, gw = pl.pallas_call(
        emit,
        out_shape=(
            jax.ShapeDtypeStruct(grad.shape, BF),
            jax.ShapeDtypeStruct(gw.shape, F32),
        ),
        in_specs=[in_any] * 2,
        out_specs=(in_any,) * 2,
        scratch_shapes=[dma((2,))],
        compiler_params=pltpu.CompilerParams(vmem_limit_bytes=4 * 2**20),
        name="emit",
    )(grad, gw)
    return (grad[None], gw)


def solution(mesh):
    return jax.shard_map(
        per_device,
        mesh=mesh,
        in_specs=(
            P("snap", "dom", None),
            P(),
            P(),
            P(),
            P(),
            P("snap", "dom", None),
            P("snap", "dom", None),
            P("snap", "dom", None, None),
            P(None, ("dom", "snap")),
            P(None, ("dom", "snap"), None),
        ),
        out_specs=(P("snap", "dom", None), P("snap", None)),
        check_vma=False,
    )
```
